512 devices in a mesh: groups: 2 (over y), ctx: 32 (over z, core), tp: 8 (over x).
Axes of the slice: x: 8, y: 2, z: 16, core: 2. Of those that a mesh axis runs over, the one named last changes fastest.
The devices are a block of a 8x8x16 slice.
Arguments:
- query_matrix: bfloat16 [8192, 8192], P(('groups', 'ctx'), 'tp'), parts along dimension 0, may hold values from -20 to 20
- key_matrix: bfloat16 [8192, 1024], P(('groups', 'ctx'), 'tp'), parts along dimension 0, may hold values from -20 to 20
- value_matrix: bfloat16 [8192, 1024], P(('groups', 'ctx'), 'tp'), parts along dimension 0, may hold values from -6 to 6
- doc_ids: int32 [8192], P('groups'), parts along dimension 0, may hold values from 0 to 5, never falling along the last dimension, each value on 1 to 2048 neighbouring positions
- out_weight: bfloat16 [8192, 4096], P('tp', 'ctx'), may hold values from -0.0625 to 0.0625
Outputs:
- projected: bfloat16 [8192, 4096], P(('groups', 'ctx'), 'tp'), parts along dimension 0
The draws below stay inside these ranges and needn't reach their ends.
There are 2 independent parts, one for each index of `groups`. The reference program is written for one: setup_inputs(seed, part) draws one part's arguments, and reference() takes and returns one part's arrays. A program takes and returns all parts, laid end to end along the dimension named above; an argument that names none is the same for every part. Nothing has to cross between parts.
Inputs may be any that keep to these rules, and one draw needn't show every extreme that they name: `doc_ids`: non-decreasing along the sequence; each document holds 1 to 2048 tokens, one exactly 2048.
All inputs are finite; a program needn't handle non-finite values.
Results may differ from the reference program's by a relative error of at most 0.015.
Values may be sent and summed in bfloat16 or wider, within the bound.
No kernel may reach another device: no remote copies, remote signals or barrier semaphores. Data moves between devices by JAX's collectives and lax.ppermute only.
A program may use at most 64 MiB of HBM per device.

```python
import math
import jax
import jax.numpy as jnp
import numpy as np
from jax import lax

QUERY_HEAD_COUNT = 64
KEY_VALUE_HEADS = 8
HEAD_SIZE = 128
DWIN = 4096
DOCS = 6
SEQUENCE_TOKENS = 4096
N_TP = 8


def draw_query_matrix(key, part):
    column_list = QUERY_HEAD_COUNT * HEAD_SIZE
    noise_key = jax.random.fold_in(key, 101)
    values = jnp.clip(1.7 * jax.random.normal(noise_key, (SEQUENCE_TOKENS, column_list)), -7.0, 7.0)
    return values.astype(jnp.bfloat16)


def draw_key_matrix(key, part):
    column_list = KEY_VALUE_HEADS * HEAD_SIZE
    noise_key = jax.random.fold_in(key, 202)
    values = jnp.clip(1.7 * jax.random.normal(noise_key, (SEQUENCE_TOKENS, column_list)), -7.0, 7.0)
    return values.astype(jnp.bfloat16)


def block_levels(key, extent, cuts, least, high):
    loudness = 1.0
    for position, shards_of in cuts:
        steps = jax.random.uniform(jax.random.fold_in(jax.random.fold_in(key, 6), position), (shards_of,), jnp.float32, least / len(cuts), high / len(cuts))
        loudness = loudness * jnp.repeat(jnp.exp(steps), extent[position] // shards_of).reshape((-1,) + (1,) * (len(extent) - 1 - position))
    return loudness


def split_up(count, total, limit, slope):
    portions = [(1 << 20) // math.isqrt(rank ** slope) + 1 for rank in range(2, count + 1)]
    surplus, holding = total - limit - (count - 1), [1] * (count - 1)
    while surplus > 0:
        free = [i for i in range(count - 1) if holding[i] < limit]
        mass, remaining = sum([portions[i] for i in free]), surplus
        for i in free:
            addition = min(limit - holding[i], max(1, remaining * portions[i] // mass), surplus)
            holding[i] = holding[i] + addition
            surplus = surplus - addition
    return np.array([limit] + holding)


def ragged_sizes(own_key, count, total, bound, lean):
    if count == 2:
        one = jax.random.randint(own_key, (), max(1, total - bound), min(bound, total - 1) + 1)
        return jnp.stack([one, total - one])
    lengths = jnp.asarray(split_up(count, total, bound, lean), jnp.int32)
    pairs = (count - 1) // 2
    giver, taker = lengths[1:1 + 2 * pairs:2], lengths[2:2 + 2 * pairs:2]
    slack = jnp.minimum(giver - 1, bound - taker)
    moved = jax.random.randint(jax.random.fold_in(own_key, 1), (pairs,), 0, 1 << 20) % (slack + 1)
    lengths = lengths.at[1:1 + 2 * pairs:2].set(giver - moved).at[2:2 + 2 * pairs:2].set(taker + moved)
    return lengths[jax.random.permutation(jax.random.fold_in(own_key, 2), count)]


def normal_values(stream_key, extent, spread, reach, cuts=(), held_as=jnp.bfloat16):
    values = spread * jax.random.normal(stream_key, extent, jnp.float32)
    if cuts:
        values = values * block_levels(stream_key, extent, cuts, -0.22, 0.18)
    return jnp.clip(values, -reach, reach).astype(held_as)


def setup_inputs(seed: int = 0, part: int = 0) -> dict:
    streams_of = jax.random.split(jax.random.key(seed), 6)
    own_keys = jax.random.split(jax.random.fold_in(streams_of[5], part), 6)
    query_matrix = draw_query_matrix(jax.random.fold_in(jax.random.fold_in(streams_of[5], part), 71), part)
    key_matrix = draw_key_matrix(jax.random.fold_in(jax.random.fold_in(streams_of[5], part), 71), part)
    value_matrix = normal_values(own_keys[2], (SEQUENCE_TOKENS, KEY_VALUE_HEADS * HEAD_SIZE), 1.0, 6.0, ((0, 32), (1, 8)))
    doc_ids = jnp.searchsorted(jnp.cumsum(ragged_sizes(own_keys[3], DOCS, SEQUENCE_TOKENS, SEQUENCE_TOKENS // 2, 0)), jnp.arange(SEQUENCE_TOKENS), side="right").astype(jnp.int32)
    out_weight = normal_values(streams_of[4], (QUERY_HEAD_COUNT * HEAD_SIZE, DWIN), (QUERY_HEAD_COUNT * HEAD_SIZE) ** -0.5, 0.0625, ((0, 8), (1, 32)))
    return dict(query_matrix=query_matrix, key_matrix=key_matrix, value_matrix=value_matrix, doc_ids=doc_ids, out_weight=out_weight)


rope_base = 1000000.0


def rotary_tables(rows, token_positions, heads):
    half_dim = HEAD_SIZE // 2
    frequency = jnp.power(jnp.float32(rope_base), -jnp.arange(half_dim, dtype=jnp.float32) * (2.0 / HEAD_SIZE))
    angles = token_positions.astype(jnp.float32)[:, None] * frequency[None, :]
    cosine = jnp.cos(angles)[:, None, :]
    sine = jnp.sin(angles)[:, None, :]
    values = rows.astype(jnp.float32).reshape(rows.shape[0], heads, HEAD_SIZE)
    first = values[..., :half_dim]
    second = values[..., half_dim:]
    turned = jnp.concatenate([first * cosine - second * sine, second * cosine + first * sine], -1)
    return turned.reshape(rows.shape[0], heads * HEAD_SIZE).astype(jnp.bfloat16)


def reference(query_matrix, key_matrix, value_matrix, doc_ids, out_weight):
    group_width = QUERY_HEAD_COUNT // KEY_VALUE_HEADS
    inverse_root = HEAD_SIZE ** -0.5
    token_positions = jnp.arange(SEQUENCE_TOKENS, dtype=jnp.int32)
    query_matrix_rot = rotary_tables(query_matrix, token_positions, QUERY_HEAD_COUNT).astype(jnp.float32).reshape(SEQUENCE_TOKENS, KEY_VALUE_HEADS, group_width, HEAD_SIZE).transpose(1, 0, 2, 3)
    every_key = rotary_tables(key_matrix, token_positions, KEY_VALUE_HEADS).astype(jnp.float32).reshape(SEQUENCE_TOKENS, KEY_VALUE_HEADS, HEAD_SIZE).transpose(1, 0, 2)
    every_value = value_matrix.astype(jnp.float32).reshape(SEQUENCE_TOKENS, KEY_VALUE_HEADS, HEAD_SIZE).transpose(1, 0, 2)
    block_rows = math.gcd(SEQUENCE_TOKENS, 512)
    block_count = SEQUENCE_TOKENS // block_rows

    def one_head(inputs):
        head_q, head_k, head_v = inputs

        def one_block(block_index):
            first_row = block_index * block_rows
            block_q = lax.dynamic_slice_in_dim(head_q, first_row, block_rows, 0)
            query_pos = first_row + jnp.arange(block_rows, dtype=jnp.int32)
            query_doc = lax.dynamic_slice_in_dim(doc_ids, first_row, block_rows, 0)
            scores = jnp.einsum("qgd,sd->gqs", block_q, head_k) * inverse_root
            allowed = ((query_doc[:, None] == doc_ids[None, :]) & (token_positions[None, :] <= query_pos[:, None]))[None]
            row_max = jnp.max(jnp.where(allowed, scores, -1e30), axis=-1, keepdims=True)
            weights = jnp.where(allowed, jnp.exp(scores - row_max), 0.0)
            totals = jnp.sum(weights, -1)
            rounded = lax.optimization_barrier(weights.astype(jnp.bfloat16)).astype(jnp.float32)
            mixed_rows = jnp.einsum("gqs,sd->qgd", rounded, head_v)
            return mixed_rows / totals.T[:, :, None]

        return lax.map(one_block, jnp.arange(block_count, dtype=jnp.int32)).reshape(SEQUENCE_TOKENS, group_width, HEAD_SIZE)

    attended = lax.map(one_head, (query_matrix_rot, every_key, every_value))
    attention = attended.transpose(1, 0, 2, 3).reshape(SEQUENCE_TOKENS, QUERY_HEAD_COUNT * HEAD_SIZE).astype(jnp.bfloat16)
    share_rows = QUERY_HEAD_COUNT * HEAD_SIZE // N_TP
    projected = jnp.zeros((SEQUENCE_TOKENS, DWIN), jnp.float32)
    for member in range(N_TP):
        partial_sum = jnp.dot(attention[:, member * share_rows:(member + 1) * share_rows],
                              out_weight[member * share_rows:(member + 1) * share_rows],
                              preferred_element_type=jnp.float32)
        projected = projected + lax.optimization_barrier(partial_sum.astype(jnp.bfloat16)).astype(jnp.float32)
    return projected.astype(jnp.bfloat16)
```

```python
import functools
import math

import jax
import jax.numpy as jnp
from jax import lax
from jax.experimental import pallas as pl
from jax.experimental.pallas import tpu as pltpu
from jax.sharding import Mesh
from jax.sharding import PartitionSpec as P

HEAD_SIZE = 128
CORES = 2


rope_base = 1000000.0


def rotary_tables(token_positions):
    half_dim = HEAD_SIZE // 2
    frequency = jnp.power(
        jnp.float32(rope_base), -jnp.arange(half_dim, dtype=jnp.float32) * (2.0 / HEAD_SIZE)
    )
    angles = token_positions.astype(jnp.float32)[:, None] * frequency[None, :]
    return jnp.cos(angles), jnp.sin(angles)


def rotate(rows, tables, heads):
    half_dim = HEAD_SIZE // 2
    cosine, sine = (t[:, None, :] for t in tables)
    values = rows.astype(jnp.float32).reshape(rows.shape[0], heads, HEAD_SIZE)
    first = values[..., :half_dim]
    second = values[..., half_dim:]
    turned = jnp.concatenate([first * cosine - second * sine, second * cosine + first * sine], -1)
    return turned.reshape(rows.shape[0], heads * HEAD_SIZE).astype(jnp.bfloat16)


def attend(heads, info, start_ref, q_ref, ka_ref, kb_ref, va_ref, vb_ref, out_ref, m_ref, l_ref, acc_ref):
    rows = q_ref.shape[0]
    first_pair, ctx = info[0], info[1]
    core = lax.rem(ctx, CORES)
    scale = HEAD_SIZE**-0.5 * math.log2(math.e)
    m_ref[...] = jnp.full(m_ref.shape, -1e30, jnp.float32)
    l_ref[...] = jnp.zeros(l_ref.shape, jnp.float32)
    acc_ref[...] = jnp.zeros(acc_ref.shape, jnp.float32)
    width = CORES * rows
    lane = lax.broadcasted_iota(jnp.int32, (rows, width), 1)
    given = ctx * rows + lax.broadcasted_iota(jnp.int32, (rows, width), 0)
    mine = lane < rows
    first = start_ref[...]

    def one_pair(step, carry):
        pair = lax.div(ctx, CORES) - step
        own = (pair * CORES + core) * rows
        other = (pair * CORES + (1 - core)) * rows - rows
        position = lane + jnp.where(mine, own, other)
        allowed = (position >= first) & (position <= given)
        keys = jnp.concatenate([ka_ref[pair], kb_ref[pair]], 0)
        values = jnp.concatenate([va_ref[pair], vb_ref[pair]], 0)
        for h in range(heads):
            q = q_ref[:, h * HEAD_SIZE : (h + 1) * HEAD_SIZE]
            scores = lax.dot_general(
                q, keys, (((1,), (1,)), ((), ())), preferred_element_type=jnp.float32
            )
            scores = jnp.where(allowed, scores, -1e30)
            old = m_ref[h]
            new = jnp.maximum(old, jnp.max(scores, 1, keepdims=True))
            weights = jnp.exp2((scores - new) * scale)
            factor = jnp.exp2((old - new) * scale)
            m_ref[h] = new
            l_ref[h] = l_ref[h] * factor + jnp.sum(weights, 1, keepdims=True)
            acc_ref[h] = acc_ref[h] * factor + jnp.dot(
                weights.astype(jnp.bfloat16), values, preferred_element_type=jnp.float32
            )
        return carry

    lax.fori_loop(0, lax.div(ctx, CORES) - first_pair + 1, one_pair, 0)
    for h in range(heads):
        out_ref[:, h * HEAD_SIZE : (h + 1) * HEAD_SIZE] = (acc_ref[h] / l_ref[h]).astype(
            jnp.bfloat16
        )


def project(count, a_ref, w_ref, out_ref):
    width = w_ref.shape[2]
    for i in range(count):
        out_ref[0, :, i * width : (i + 1) * width] = jnp.dot(
            a_ref[...], w_ref[i], preferred_element_type=jnp.float32
        ).astype(jnp.bfloat16)


def on_device(query_matrix, key_matrix, value_matrix, doc_ids, out_weight):
    tok_rows = query_matrix.shape[0]
    query_heads = query_matrix.shape[1] // HEAD_SIZE
    members = lax.axis_size("tp")
    ctx_index = lax.axis_index("z") * CORES + lax.axis_index("core")
    weight_blocks = lax.all_gather(out_weight, ("z", "core"), axis=0, tiled=False)
    given_pos = ctx_index * tok_rows + jnp.arange(tok_rows, dtype=jnp.int32)
    tables = rotary_tables(given_pos)
    keys_here = rotate(key_matrix, tables, 1)
    swap = [(i, CORES - 1 - i) for i in range(CORES)]
    keys_a = lax.all_gather(keys_here, "z", axis=0, tiled=False)
    keys_b = lax.ppermute(keys_a, "core", swap)
    values_a = lax.all_gather(value_matrix, "z", axis=0, tiled=False)
    values_b = lax.ppermute(values_a, "core", swap)
    queries = rotate(query_matrix, tables, query_heads)
    query_doc = lax.dynamic_slice_in_dim(doc_ids, ctx_index * tok_rows, tok_rows, 0)
    starts = jnp.sum((doc_ids[None, :] < query_doc[:, None]).astype(jnp.int32), 1)
    first_pair = jnp.min(starts) // (CORES * tok_rows)
    info = jnp.stack([first_pair, ctx_index]).astype(jnp.int32)
    vmem = pl.BlockSpec(memory_space=pltpu.VMEM)
    attention = pl.pallas_call(
        functools.partial(attend, query_heads),
        out_shape=jax.ShapeDtypeStruct((tok_rows, query_heads * HEAD_SIZE), jnp.bfloat16),
        in_specs=[pl.BlockSpec(memory_space=pltpu.SMEM)] + [vmem] * 6,
        out_specs=vmem,
        scratch_shapes=[
            pltpu.VMEM((query_heads, tok_rows, 1), jnp.float32),
            pltpu.VMEM((query_heads, tok_rows, 1), jnp.float32),
            pltpu.VMEM((query_heads, tok_rows, HEAD_SIZE), jnp.float32),
        ],
        cost_estimate=pl.CostEstimate(flops=2 * 10**9, bytes_accessed=3 * 10**6, transcendentals=10**6),
        name="attend",
    )(info, starts[:, None], queries, keys_a, keys_b, values_a, values_b)
    blocks, depth, width = weight_blocks.shape
    share = blocks // members
    terms = pl.pallas_call(
        functools.partial(project, share),
        grid=(members,),
        out_shape=jax.ShapeDtypeStruct((members, tok_rows, share * width), jnp.bfloat16),
        in_specs=[
            pl.BlockSpec((tok_rows, depth), lambda i: (0, 0)),
            pl.BlockSpec((share, depth, width), lambda i: (i, 0, 0)),
        ],
        out_specs=pl.BlockSpec((1, tok_rows, share * width), lambda i: (i, 0, 0)),
        cost_estimate=pl.CostEstimate(flops=10**9, bytes_accessed=10**7, transcendentals=0),
        name="project",
    )(attention, weight_blocks)
    arrived = lax.all_to_all(terms, "tp", split_axis=0, concat_axis=0, tiled=True)
    return arrived.astype(jnp.float32).sum(axis=0).astype(jnp.bfloat16)


def solution(mesh):
    groups, ctx, tp = mesh.devices.shape
    fine = Mesh(mesh.devices.reshape(groups, ctx // CORES, CORES, tp), ("groups", "z", "core", "tp"))
    tokens = ("groups", "z", "core")
    in_specs = (P(tokens, "tp"), P(tokens, "tp"), P(tokens, "tp"), P("groups"), P("tp", ("z", "core")))
    return jax.shard_map(
        on_device, mesh=fine, in_specs=in_specs, out_specs=P(tokens, "tp"), check_vma=False
    )
```

```python
import functools
import math

import jax
import jax.numpy as jnp
from jax import lax
from jax.experimental import pallas as pl
from jax.experimental.pallas import tpu as pltpu
from jax.sharding import Mesh
from jax.sharding import PartitionSpec as P

HEAD_SIZE = 128
CORES = 2
DOCS = 6


rope_base = 1000000.0


def rotary_tables(token_positions):
    half_dim = HEAD_SIZE // 2
    lane = jnp.arange(HEAD_SIZE, dtype=jnp.int32)
    power = -(lane % half_dim).astype(jnp.float32) * (2.0 / HEAD_SIZE)
    angles = token_positions.astype(jnp.float32)[:, None] * jnp.power(jnp.float32(rope_base), power)
    return jnp.cos(angles), jnp.where(lane < half_dim, -1.0, 1.0) * jnp.sin(angles)


def prepare(heads, cosine_ref, sine_ref, q_ref, k_ref, v_ref, q_out, k_out, v_out):
    cosine, sine = cosine_ref[...], sine_ref[...]

    def turned(x):
        x = x.astype(jnp.float32)
        return (x * cosine + pltpu.roll(x, HEAD_SIZE // 2, 1) * sine).astype(jnp.bfloat16)

    k_out[...] = turned(k_ref[...])
    v_out[...] = v_ref[...].astype(jnp.float32).T.astype(jnp.bfloat16)
    for h in range(heads):
        at = slice(h * HEAD_SIZE, (h + 1) * HEAD_SIZE)
        q_out[:, at] = turned(q_ref[:, at])


def attend(heads, info, doc_ref, q_ref, ka_ref, kb_ref, va_ref, vb_ref, out_ref, m_ref, l_ref, acc_ref):
    rows = q_ref.shape[0]
    ctx = info[0]
    core = lax.rem(ctx, CORES)
    scale = HEAD_SIZE**-0.5 * math.log2(math.e)
    m_ref[...] = jnp.full(m_ref.shape, -1e30, jnp.float32)
    l_ref[...] = jnp.zeros(l_ref.shape, jnp.float32)
    acc_ref[...] = jnp.zeros(acc_ref.shape, jnp.float32)
    width = CORES * rows
    key = lax.broadcasted_iota(jnp.int32, (width, rows), 0)
    given = ctx * rows + lax.broadcasted_iota(jnp.int32, (width, rows), 1)
    mine = key < rows
    docs, here = doc_ref[...], doc_ref[pl.ds(ctx, 1), :]
    first = jnp.zeros(here.shape, jnp.int32)
    for d in range(1, DOCS):
        before = jnp.sum((docs < d).astype(jnp.int32), keepdims=True)
        first = first + jnp.where(here == d, before, 0)
    first_pair = lax.div(jnp.min(first), width)

    def one_pair(step, carry):
        pair = lax.div(ctx, CORES) - step
        own = (pair * CORES + core) * rows
        other = (pair * CORES + (1 - core)) * rows - rows
        position = key + jnp.where(mine, own, other)
        allowed = (position >= first) & (position <= given)
        keys = jnp.concatenate([ka_ref[pair], kb_ref[pair]], 0)
        values = jnp.concatenate([va_ref[pair], vb_ref[pair]], 1)
        for h in range(heads):
            q = q_ref[:, h * HEAD_SIZE : (h + 1) * HEAD_SIZE]
            scores = lax.dot_general(
                keys, q, (((1,), (1,)), ((), ())), preferred_element_type=jnp.float32
            )
            scores = jnp.where(allowed, scores, -1e30)
            old = m_ref[h]
            new = jnp.maximum(old, jnp.max(scores, 0, keepdims=True))
            weights = jnp.exp2((scores - new) * scale)
            factor = jnp.exp2((old - new) * scale)
            m_ref[h] = new
            l_ref[h] = l_ref[h] * factor + jnp.sum(weights, 0, keepdims=True)
            acc_ref[h] = acc_ref[h] * factor + jnp.dot(
                values, weights.astype(jnp.bfloat16), preferred_element_type=jnp.float32
            )
        return carry

    lax.fori_loop(0, lax.div(ctx, CORES) - first_pair + 1, one_pair, 0)
    for h in range(heads):
        out_ref[:, h * HEAD_SIZE : (h + 1) * HEAD_SIZE] = (
            (acc_ref[h] / l_ref[h]).T.astype(jnp.bfloat16)
        )


def project(count, a_ref, w_ref, out_ref):
    weights = jnp.concatenate([w_ref[i] for i in range(count)], 1)
    out_ref[0] = jnp.dot(a_ref[...], weights, preferred_element_type=jnp.float32).astype(
        jnp.bfloat16
    )


def on_device(query_matrix, key_matrix, value_matrix, doc_ids, out_weight):
    tok_rows = query_matrix.shape[0]
    query_heads = query_matrix.shape[1] // HEAD_SIZE
    members = lax.axis_size("tp")
    ctx_index = lax.axis_index("z") * CORES + lax.axis_index("core")
    weight_blocks = lax.all_gather(out_weight, ("z", "core"), axis=0, tiled=False)
    given_pos = ctx_index * tok_rows + jnp.arange(tok_rows, dtype=jnp.int32)
    vmem = pl.BlockSpec(memory_space=pltpu.VMEM)
    queries, keys_here, values_here = pl.pallas_call(
        functools.partial(prepare, query_heads),
        out_shape=(
            jax.ShapeDtypeStruct(query_matrix.shape, jnp.bfloat16),
            jax.ShapeDtypeStruct(key_matrix.shape, jnp.bfloat16),
            jax.ShapeDtypeStruct(value_matrix.shape[::-1], jnp.bfloat16),
        ),
        in_specs=[vmem] * 5,
        out_specs=(vmem,) * 3,
        compiler_params=pltpu.CompilerParams(vmem_limit_bytes=16 * 2**20),
        cost_estimate=pl.CostEstimate(flops=10**6, bytes_accessed=10**6, transcendentals=0),
        name="prepare",
    )(*rotary_tables(given_pos), query_matrix, key_matrix, value_matrix)
    swap = [(i, CORES - 1 - i) for i in range(CORES)]
    keys_a = lax.all_gather(keys_here, "z", axis=0, tiled=False)
    keys_b = lax.ppermute(keys_a, "core", swap)
    values_a = lax.all_gather(values_here, "z", axis=0, tiled=False)
    values_b = lax.ppermute(values_a, "core", swap)
    info = ctx_index.astype(jnp.int32).reshape(1)
    docs = doc_ids.reshape(-1, tok_rows)
    attention = pl.pallas_call(
        functools.partial(attend, query_heads),
        out_shape=jax.ShapeDtypeStruct((tok_rows, query_heads * HEAD_SIZE), jnp.bfloat16),
        in_specs=[pl.BlockSpec(memory_space=pltpu.SMEM)] + [vmem] * 6,
        out_specs=vmem,
        scratch_shapes=[
            pltpu.VMEM((query_heads, 1, tok_rows), jnp.float32),
            pltpu.VMEM((query_heads, 1, tok_rows), jnp.float32),
            pltpu.VMEM((query_heads, tok_rows, HEAD_SIZE), jnp.float32),
        ],
        cost_estimate=pl.CostEstimate(flops=2 * 10**9, bytes_accessed=3 * 10**6, transcendentals=10**6),
        compiler_params=pltpu.CompilerParams(vmem_limit_bytes=16 * 2**20),
        name="attend",
    )(info, docs, queries, keys_a, keys_b, values_a, values_b)
    blocks, depth, width = weight_blocks.shape
    share = blocks // members
    terms = pl.pallas_call(
        functools.partial(project, share),
        grid=(members,),
        out_shape=jax.ShapeDtypeStruct((members, tok_rows, share * width), jnp.bfloat16),
        in_specs=[
            pl.BlockSpec((tok_rows, depth), lambda i: (0, 0)),
            pl.BlockSpec((share, depth, width), lambda i: (i, 0, 0)),
        ],
        out_specs=pl.BlockSpec((1, tok_rows, share * width), lambda i: (i, 0, 0)),
        cost_estimate=pl.CostEstimate(flops=10**9, bytes_accessed=10**7, transcendentals=0),
        name="project",
    )(attention, weight_blocks)
    arrived = lax.all_to_all(terms, "tp", split_axis=0, concat_axis=0, tiled=True)
    return arrived.astype(jnp.float32).sum(axis=0).astype(jnp.bfloat16)


def solution(mesh):
    groups, ctx, tp = mesh.devices.shape
    fine = Mesh(mesh.devices.reshape(groups, ctx // CORES, CORES, tp), ("groups", "z", "core", "tp"))
    tokens = ("groups", "z", "core")
    in_specs = (P(tokens, "tp"), P(tokens, "tp"), P(tokens, "tp"), P("groups"), P("tp", ("z", "core")))
    return jax.shard_map(
        on_device, mesh=fine, in_specs=in_specs, out_specs=P(tokens, "tp"), check_vma=False
    )
```

```python
import functools
import math

import jax
import jax.numpy as jnp
from jax import lax
from jax.experimental import pallas as pl
from jax.experimental.pallas import tpu as pltpu
from jax.sharding import Mesh
from jax.sharding import PartitionSpec as P

HEAD_SIZE = 128
CORES = 2
DOCS = 6
MAX_DOC = 2048


rope_base = 1000000.0


def rotary_tables(token_positions):
    half_dim = HEAD_SIZE // 2
    lane = jnp.arange(HEAD_SIZE, dtype=jnp.int32)
    power = -(lane % half_dim).astype(jnp.float32) * (2.0 / HEAD_SIZE)
    angles = token_positions.astype(jnp.float32)[:, None] * jnp.power(jnp.float32(rope_base), power)
    return jnp.cos(angles), jnp.where(lane < half_dim, -1.0, 1.0) * jnp.sin(angles)


def prepare(heads, cosine_ref, sine_ref, q_ref, k_ref, v_ref, q_out, kv_out):
    cosine, sine = cosine_ref[...], sine_ref[...]

    def turned(x):
        x = x.astype(jnp.float32)
        return (x * cosine + pltpu.roll(x, HEAD_SIZE // 2, 1) * sine).astype(jnp.bfloat16)

    kv_out[0] = turned(k_ref[...])
    kv_out[1] = v_ref[...].astype(jnp.float32).T.astype(jnp.bfloat16)
    for h in range(heads):
        at = slice(h * HEAD_SIZE, (h + 1) * HEAD_SIZE)
        q_out[:, at] = turned(q_ref[:, at])


def attend(heads, info, doc_ref, q_ref, a_ref, b_ref, out_ref, m_ref, l_ref, acc_ref):
    rows = q_ref.shape[0]
    line = a_ref.shape[0]
    ctx = info[0]
    core = lax.rem(ctx, CORES)
    chip = lax.div(ctx, CORES)
    scale = HEAD_SIZE**-0.5 * math.log2(math.e)
    m_ref[...] = jnp.full(m_ref.shape, -1e30, jnp.float32)
    l_ref[...] = jnp.zeros(l_ref.shape, jnp.float32)
    acc_ref[...] = jnp.zeros(acc_ref.shape, jnp.float32)
    width = CORES * rows
    key = lax.broadcasted_iota(jnp.int32, (width, rows), 0)
    given = ctx * rows + lax.broadcasted_iota(jnp.int32, (width, rows), 1)
    mine = key < rows
    docs, here = doc_ref[...], doc_ref[pl.ds(ctx, 1), :]
    first = jnp.zeros(here.shape, jnp.int32)
    for d in range(1, DOCS):
        before = jnp.sum((docs < d).astype(jnp.int32), keepdims=True)
        first = first + jnp.where(here == d, before, 0)
    first_chip = lax.div(jnp.min(first), width)

    def one_chip(step, carry):
        at = chip - step
        own = (at * CORES + core) * rows
        other = (at * CORES + (1 - core)) * rows - rows
        position = key + jnp.where(mine, own, other)
        allowed = (position >= first) & (position <= given)
        member, back = lax.rem(at, line), lax.div(chip, line) - lax.div(at, line)
        keys = jnp.concatenate([a_ref[member, back, 0], b_ref[member, back, 0]], 0)
        values = jnp.concatenate([a_ref[member, back, 1], b_ref[member, back, 1]], 1)
        for h in range(heads):
            q = q_ref[:, h * HEAD_SIZE : (h + 1) * HEAD_SIZE]
            scores = lax.dot_general(
                keys, q, (((1,), (1,)), ((), ())), preferred_element_type=jnp.float32
            )
            scores = jnp.where(allowed, scores, -1e30)
            old = m_ref[h]
            new = jnp.maximum(old, jnp.max(scores, 0, keepdims=True))
            weights = jnp.exp2((scores - new) * scale)
            factor = jnp.exp2((old - new) * scale)
            m_ref[h] = new
            l_ref[h] = l_ref[h] * factor + jnp.sum(weights, 0, keepdims=True)
            acc_ref[h] = acc_ref[h] * factor + jnp.dot(
                values, weights.astype(jnp.bfloat16), preferred_element_type=jnp.float32
            )
        return carry

    lax.fori_loop(0, chip - first_chip + 1, one_chip, 0)
    for h in range(heads):
        out_ref[:, h * HEAD_SIZE : (h + 1) * HEAD_SIZE] = (
            (acc_ref[h] / l_ref[h]).T.astype(jnp.bfloat16)
        )


def project(count, level_ref, own_ref, other_ref, *refs):
    out_ref = refs[count]
    rows = own_ref.shape[0]
    weights = jnp.concatenate([w_ref[0] for w_ref in refs[:count]], 1)
    for i, a_ref in enumerate((own_ref, other_ref)):
        out_ref[0, i * rows : (i + 1) * rows] = jnp.dot(
            a_ref[...], weights, preferred_element_type=jnp.float32
        ).astype(jnp.bfloat16)


def total(terms_ref, kept_ref, sent_ref):
    rows = kept_ref.shape[0]
    for i, out_ref in enumerate((kept_ref, sent_ref)):
        at = slice(i * rows, (i + 1) * rows)
        out_ref[...] = jnp.sum(terms_ref[:, at].astype(jnp.float32), 0).astype(jnp.bfloat16)


def weave(count, core, kept_ref, given_ref, out_ref):
    width = kept_ref.shape[1] // count
    even = core[0] == 0
    for j in range(count):
        kept, given = (r[:, j * width : (j + 1) * width] for r in (kept_ref, given_ref))
        at = j * CORES * width
        out_ref[:, at : at + width] = jnp.where(even, kept, given)
        out_ref[:, at + width : at + CORES * width] = jnp.where(even, given, kept)


def on_device(query_matrix, key_matrix, value_matrix, doc_ids, out_weight):
    tok_rows = query_matrix.shape[0]
    query_heads = query_matrix.shape[1] // HEAD_SIZE
    members = lax.axis_size("tp")
    lines, line = lax.axis_size("far"), lax.axis_size("near")
    core = lax.axis_index("core")
    my_line = lax.axis_index("far")
    ctx_index = (my_line * line + lax.axis_index("near")) * CORES + core
    weight_blocks = lax.all_gather(out_weight, ("far", "near"), axis=0, tiled=False)
    given_pos = ctx_index * tok_rows + jnp.arange(tok_rows, dtype=jnp.int32)
    vmem = pl.BlockSpec(memory_space=pltpu.VMEM)
    small = pltpu.CompilerParams(vmem_limit_bytes=16 * 2**20)
    queries, here = pl.pallas_call(
        functools.partial(prepare, query_heads),
        out_shape=(
            jax.ShapeDtypeStruct(query_matrix.shape, jnp.bfloat16),
            jax.ShapeDtypeStruct((2,) + key_matrix.shape, jnp.bfloat16),
        ),
        in_specs=[vmem] * 5,
        out_specs=(vmem,) * 2,
        compiler_params=small,
        cost_estimate=pl.CostEstimate(flops=10**6, bytes_accessed=10**6, transcendentals=0),
        name="prepare",
    )(*rotary_tables(given_pos), query_matrix, key_matrix, value_matrix)
    swap = [(i, CORES - 1 - i) for i in range(CORES)]
    far = lax.all_gather(here, "far", axis=0, tiled=False)
    back = min(lines, 1 + -(-(MAX_DOC - 1) // (line * CORES * tok_rows)))
    wanted = jnp.stack(
        [
            lax.dynamic_index_in_dim(far, (my_line - i) % lines, 0, keepdims=False)
            for i in range(back)
        ]
    )
    mine = lax.all_gather(wanted, "near", axis=0, tiled=False)
    theirs = lax.ppermute(mine, "core", swap)
    info = ctx_index.astype(jnp.int32).reshape(1)
    docs = doc_ids.reshape(-1, tok_rows)
    attention = pl.pallas_call(
        functools.partial(attend, query_heads),
        out_shape=jax.ShapeDtypeStruct((tok_rows, query_heads * HEAD_SIZE), jnp.bfloat16),
        in_specs=[pl.BlockSpec(memory_space=pltpu.SMEM)] + [vmem] * 4,
        out_specs=vmem,
        scratch_shapes=[
            pltpu.VMEM((query_heads, 1, tok_rows), jnp.float32),
            pltpu.VMEM((query_heads, 1, tok_rows), jnp.float32),
            pltpu.VMEM((query_heads, HEAD_SIZE, tok_rows), jnp.float32),
        ],
        cost_estimate=pl.CostEstimate(flops=2 * 10**9, bytes_accessed=3 * 10**6, transcendentals=10**6),
        compiler_params=small,
        name="attend",
    )(info, docs, queries, mine, theirs)
    level = lax.all_to_all(
        attention[: members * 8, :HEAD_SIZE].reshape(members, 8, HEAD_SIZE),
        "tp",
        split_axis=0,
        concat_axis=0,
        tiled=True,
    )
    attention_other = lax.ppermute(attention, "core", swap)
    blocks, depth, width = weight_blocks.shape
    share = blocks // members
    whole = pl.BlockSpec((tok_rows, depth), lambda i: (0, 0))
    terms = pl.pallas_call(
        functools.partial(project, share),
        grid=(members,),
        out_shape=jax.ShapeDtypeStruct((members, CORES * tok_rows, share * width), jnp.bfloat16),
        in_specs=[pl.BlockSpec(memory_space=pl.ANY), whole, whole]
        + [
            pl.BlockSpec((1, depth, width), lambda i, j=j: (i * share + j, 0, 0))
            for j in range(share)
        ],
        out_specs=pl.BlockSpec((1, CORES * tok_rows, share * width), lambda i: (i, 0, 0)),
        cost_estimate=pl.CostEstimate(flops=10**9, bytes_accessed=10**7, transcendentals=0),
        name="project",
    )(level, attention, attention_other, *[weight_blocks] * share)
    arrived = lax.all_to_all(terms, "tp", split_axis=0, concat_axis=0, tiled=True)
    half = jax.ShapeDtypeStruct((tok_rows, share * width), jnp.bfloat16)
    kept, sent = pl.pallas_call(
        total,
        out_shape=(half, half),
        in_specs=[vmem],
        out_specs=(vmem, vmem),
        compiler_params=small,
        name="total",
    )(arrived)
    given = lax.ppermute(sent, "core", swap)
    return pl.pallas_call(
        functools.partial(weave, share),
        out_shape=jax.ShapeDtypeStruct((tok_rows, share * CORES * width), jnp.bfloat16),
        in_specs=[pl.BlockSpec(memory_space=pltpu.SMEM), vmem, vmem],
        out_specs=vmem,
        compiler_params=small,
        name="weave",
    )(core.astype(jnp.int32).reshape(1), kept, given)


def solution(mesh):
    groups, ctx, tp = mesh.devices.shape
    near = math.gcd(ctx // CORES, 4)
    far = ctx // CORES // near
    names = ("groups", "far", "near", "core", "tp")
    fine = Mesh(mesh.devices.reshape(groups, far, near, CORES, tp), names)
    ctx_axes = ("far", "near", "core")
    tokens = ("groups",) + ctx_axes
    in_specs = (P(tokens, "tp"), P(tokens, "tp"), P(tokens, "tp"), P("groups"), P("tp", ctx_axes))
    return jax.shard_map(
        on_device, mesh=fine, in_specs=in_specs, out_specs=P(tokens, "tp"), check_vma=False
    )
```

```python
import functools
import math

import jax
import jax.numpy as jnp
from jax import lax
from jax.experimental import pallas as pl
from jax.experimental.pallas import tpu as pltpu
from jax.sharding import Mesh
from jax.sharding import PartitionSpec as P

HEAD_SIZE = 128
CORES = 2
DOCS = 6
MAX_DOC = 2048


rope_base = 1000000.0


def rotary_tables(token_positions):
    half_dim = HEAD_SIZE // 2
    lane = jnp.arange(HEAD_SIZE, dtype=jnp.int32)
    power = -(lane % half_dim).astype(jnp.float32) * (2.0 / HEAD_SIZE)
    angles = token_positions.astype(jnp.float32)[:, None] * jnp.power(jnp.float32(rope_base), power)
    return jnp.cos(angles), jnp.where(lane < half_dim, -1.0, 1.0) * jnp.sin(angles)


def prepare(heads, cosine_ref, sine_ref, q_ref, k_ref, v_ref, q_out, kv_out):
    cosine, sine = cosine_ref[...], sine_ref[...]

    def turned(x):
        x = x.astype(jnp.float32)
        return (x * cosine + pltpu.roll(x, HEAD_SIZE // 2, 1) * sine).astype(jnp.bfloat16)

    kv_out[0] = turned(k_ref[...])
    kv_out[1] = v_ref[...].astype(jnp.float32).T.astype(jnp.bfloat16)
    for h in range(heads):
        at = slice(h * HEAD_SIZE, (h + 1) * HEAD_SIZE)
        q_out[:, at] = turned(q_ref[:, at])


def attend(heads, info, doc_ref, q_ref, a_ref, b_ref, out_ref, m_ref, l_ref, acc_ref):
    rows = q_ref.shape[0]
    line = a_ref.shape[0]
    ctx = info[0]
    core = lax.rem(ctx, CORES)
    chip = lax.div(ctx, CORES)
    scale = HEAD_SIZE**-0.5 * math.log2(math.e)
    m_ref[...] = jnp.full(m_ref.shape, -1e30, jnp.float32)
    l_ref[...] = jnp.zeros(l_ref.shape, jnp.float32)
    acc_ref[...] = jnp.zeros(acc_ref.shape, jnp.float32)
    width = CORES * rows
    key = lax.broadcasted_iota(jnp.int32, (width, rows), 0)
    given = ctx * rows + lax.broadcasted_iota(jnp.int32, (width, rows), 1)
    mine = key < rows
    docs, here = doc_ref[...], doc_ref[pl.ds(ctx, 1), :]
    first = jnp.zeros(here.shape, jnp.int32)
    for d in range(1, DOCS):
        before = jnp.sum((docs < d).astype(jnp.int32), keepdims=True)
        first = first + jnp.where(here == d, before, 0)
    first_chip = lax.div(jnp.min(first), width)

    def one_chip(step, carry):
        at = chip - step
        own = (at * CORES + core) * rows
        other = (at * CORES + (1 - core)) * rows - rows
        position = key + jnp.where(mine, own, other)
        allowed = (position >= first) & (position <= given)
        member, back = lax.rem(at, line), lax.div(chip, line) - lax.div(at, line)
        keys = jnp.concatenate([a_ref[member, back, 0], b_ref[member, back, 0]], 0)
        values = jnp.concatenate([a_ref[member, back, 1], b_ref[member, back, 1]], 1)
        for h in range(heads):
            q = q_ref[:, h * HEAD_SIZE : (h + 1) * HEAD_SIZE]
            scores = lax.dot_general(
                keys, q, (((1,), (1,)), ((), ())), preferred_element_type=jnp.float32
            )
            scores = jnp.where(allowed, scores, -1e30)
            old = m_ref[h]
            new = jnp.maximum(old, jnp.max(scores, 0, keepdims=True))
            weights = jnp.exp2((scores - new) * scale)
            factor = jnp.exp2((old - new) * scale)
            m_ref[h] = new
            l_ref[h] = l_ref[h] * factor + jnp.sum(weights, 0, keepdims=True)
            acc_ref[h] = acc_ref[h] * factor + jnp.dot(
                values, weights.astype(jnp.bfloat16), preferred_element_type=jnp.float32
            )
        return carry

    lax.fori_loop(0, chip - first_chip + 1, one_chip, 0)
    for h in range(heads):
        out_ref[:, h * HEAD_SIZE : (h + 1) * HEAD_SIZE] = (
            (acc_ref[h] / l_ref[h]).T.astype(jnp.bfloat16)
        )


def project(count, parts, level_ref, a_ref, *refs):
    out_ref = refs[count]
    width = out_ref.shape[2]
    weights = jnp.concatenate([w_ref[0] for w_ref in refs[:count]], 1)
    terms = jnp.dot(a_ref[...], weights, preferred_element_type=jnp.float32).astype(jnp.bfloat16)
    for i in range(parts):
        out_ref[i] = terms[:, i * width : (i + 1) * width]


def on_device(query_matrix, key_matrix, value_matrix, doc_ids, out_weight):
    tok_rows = query_matrix.shape[0]
    query_heads = query_matrix.shape[1] // HEAD_SIZE
    members = lax.axis_size("tp")
    lines, line = lax.axis_size("far"), lax.axis_size("near")
    core = lax.axis_index("core")
    my_line = lax.axis_index("far")
    ctx_index = (my_line * line + lax.axis_index("near")) * CORES + core
    weight_blocks = lax.all_gather(out_weight, ("far", "near", "core"), axis=0, tiled=False)
    given_pos = ctx_index * tok_rows + jnp.arange(tok_rows, dtype=jnp.int32)
    vmem = pl.BlockSpec(memory_space=pltpu.VMEM)
    small = pltpu.CompilerParams(vmem_limit_bytes=16 * 2**20)
    queries, here = pl.pallas_call(
        functools.partial(prepare, query_heads),
        out_shape=(
            jax.ShapeDtypeStruct(query_matrix.shape, jnp.bfloat16),
            jax.ShapeDtypeStruct((2,) + key_matrix.shape, jnp.bfloat16),
        ),
        in_specs=[vmem] * 5,
        out_specs=(vmem,) * 2,
        compiler_params=small,
        cost_estimate=pl.CostEstimate(flops=10**6, bytes_accessed=10**6, transcendentals=0),
        name="prepare",
    )(*rotary_tables(given_pos), query_matrix, key_matrix, value_matrix)
    swap = [(i, CORES - 1 - i) for i in range(CORES)]
    far = lax.all_gather(here, "far", axis=0, tiled=False)
    back = min(lines, 1 + -(-(MAX_DOC - 1) // (line * CORES * tok_rows)))
    wanted = jnp.stack(
        [
            lax.dynamic_index_in_dim(far, (my_line - i) % lines, 0, keepdims=False)
            for i in range(back)
        ]
    )
    mine = lax.all_gather(wanted, "near", axis=0, tiled=False)
    theirs = lax.ppermute(mine, "core", swap)
    info = ctx_index.astype(jnp.int32).reshape(1)
    docs = doc_ids.reshape(-1, tok_rows)
    attention = pl.pallas_call(
        functools.partial(attend, query_heads),
        out_shape=jax.ShapeDtypeStruct((tok_rows, query_heads * HEAD_SIZE), jnp.bfloat16),
        in_specs=[pl.BlockSpec(memory_space=pltpu.SMEM)] + [vmem] * 4,
        out_specs=vmem,
        scratch_shapes=[
            pltpu.VMEM((query_heads, 1, tok_rows), jnp.float32),
            pltpu.VMEM((query_heads, 1, tok_rows), jnp.float32),
            pltpu.VMEM((query_heads, HEAD_SIZE, tok_rows), jnp.float32),
        ],
        cost_estimate=pl.CostEstimate(flops=2 * 10**9, bytes_accessed=3 * 10**6, transcendentals=10**6),
        compiler_params=small,
        name="attend",
    )(info, docs, queries, mine, theirs)
    level = lax.all_to_all(
        attention[: members * 8, :HEAD_SIZE].reshape(members, 8, HEAD_SIZE),
        "tp",
        split_axis=0,
        concat_axis=0,
        tiled=True,
    )
    blocks, depth, width = weight_blocks.shape
    share = blocks // members
    parts = math.gcd(members, 2)
    count = share * parts
    terms = pl.pallas_call(
        functools.partial(project, count, parts),
        grid=(blocks // count,),
        out_shape=jax.ShapeDtypeStruct((members, tok_rows, share * width), jnp.bfloat16),
        in_specs=[pl.BlockSpec(memory_space=pl.ANY), pl.BlockSpec((tok_rows, depth), lambda i: (0, 0))]
        + [
            pl.BlockSpec((1, depth, width), lambda i, j=j: (i * count + j, 0, 0))
            for j in range(count)
        ],
        out_specs=pl.BlockSpec((parts, tok_rows, share * width), lambda i: (i, 0, 0)),
        cost_estimate=pl.CostEstimate(flops=10**9, bytes_accessed=10**7, transcendentals=0),
        name="project",
    )(level, attention, *[weight_blocks] * count)
    arrived = lax.all_to_all(terms, "tp", split_axis=0, concat_axis=0, tiled=True)
    return arrived.astype(jnp.float32).sum(axis=0).astype(jnp.bfloat16)


def solution(mesh):
    groups, ctx, tp = mesh.devices.shape
    near = math.gcd(ctx // CORES, 4)
    far = ctx // CORES // near
    names = ("groups", "far", "near", "core", "tp")
    fine = Mesh(mesh.devices.reshape(groups, far, near, CORES, tp), names)
    ctx_axes = ("far", "near", "core")
    tokens = ("groups",) + ctx_axes
    in_specs = (P(tokens, "tp"), P(tokens, "tp"), P(tokens, "tp"), P("groups"), P("tp", ctx_axes))
    return jax.shard_map(
        on_device, mesh=fine, in_specs=in_specs, out_specs=P(tokens, "tp"), check_vma=False
    )
```

```python
import functools
import math

import jax
import jax.numpy as jnp
from jax import lax
from jax.experimental import pallas as pl
from jax.experimental.pallas import tpu as pltpu
from jax.sharding import Mesh
from jax.sharding import PartitionSpec as P

HEAD_SIZE = 128
CORES = 2
DOCS = 6


rope_base = 1000000.0


def rotary_tables(token_positions):
    half_dim = HEAD_SIZE // 2
    lane = jnp.arange(HEAD_SIZE, dtype=jnp.int32)
    power = -(lane % half_dim).astype(jnp.float32) * (2.0 / HEAD_SIZE)
    angles = token_positions.astype(jnp.float32)[:, None] * jnp.power(jnp.float32(rope_base), power)
    return jnp.cos(angles), jnp.where(lane < half_dim, -1.0, 1.0) * jnp.sin(angles)


def prepare(heads, info, cosine_ref, sine_ref, q_hbm, k_hbm, v_hbm, doc_hbm, q_out, k_out, v_out, first_out, q_ref, k_ref, v_ref, doc_ref, sems):
    pairs = ((k_hbm, k_ref), (v_hbm, v_ref), (q_hbm, q_ref), (doc_hbm, doc_ref))
    copies = [pltpu.make_async_copy(a, b, sems.at[i]) for i, (a, b) in enumerate(pairs)]
    for copy in copies:
        copy.start()
    cosine, sine = cosine_ref[...], sine_ref[...]

    def turned(x):
        x = x.astype(jnp.float32)
        return (x * cosine + pltpu.roll(x, HEAD_SIZE // 2, 1) * sine).astype(jnp.bfloat16)

    copies[0].wait()
    k_out[...] = turned(k_ref[...])
    copies[1].wait()
    v_out[...] = v_ref[...].astype(jnp.float32).T.astype(jnp.bfloat16)
    copies[2].wait()
    for h in range(heads):
        q_out[h] = turned(q_ref[:, h * HEAD_SIZE : (h + 1) * HEAD_SIZE])
    copies[3].wait()
    docs, here = doc_ref[...], doc_ref[pl.ds(info[0], 1), :]
    first = jnp.zeros(here.shape, jnp.int32)
    for d in range(1, DOCS):
        before = jnp.sum((docs < d).astype(jnp.int32), keepdims=True)
        first = first + jnp.where(here == d, before, 0)
    first_out[...] = jnp.broadcast_to(first, first_out.shape)


def attend(heads, together, info, first_ref, q_ref, ka_ref, kb_ref, va_ref, vb_ref, out_ref, m_ref, l_ref, acc_ref):
    rows = ka_ref.shape[1]
    ctx = info[0]
    core = lax.rem(ctx, CORES)
    chip = lax.div(ctx, CORES)
    scale = HEAD_SIZE**-0.5 * math.log2(math.e)
    m_ref[...] = jnp.full(m_ref.shape, -1e30, jnp.float32)
    l_ref[...] = jnp.zeros(l_ref.shape, jnp.float32)
    acc_ref[...] = jnp.zeros(acc_ref.shape, jnp.float32)
    width = CORES * rows
    key = lax.broadcasted_iota(jnp.int32, (width, rows), 0)
    given = ctx * rows + lax.broadcasted_iota(jnp.int32, (width, rows), 1)
    mine = key < rows
    first = first_ref[0:1, :]
    first_chip = lax.div(jnp.min(first), width)

    def one_chip(step, carry):
        at = chip - step
        own = (at * CORES + core) * rows
        other = (at * CORES + (1 - core)) * rows - rows
        position = key + jnp.where(mine, own, other)
        bias = jnp.where((position >= first) & (position <= given), 0.0, -1e30)
        bias = jnp.concatenate([bias] * together, 1)
        keys = jnp.concatenate([ka_ref[at], kb_ref[at]], 0)
        values = jnp.concatenate([va_ref[at], vb_ref[at]], 1)
        for g in range(heads // together):
            q = q_ref[g * together : (g + 1) * together].reshape(together * rows, HEAD_SIZE)
            scores = lax.dot_general(
                keys, q, (((1,), (1,)), ((), ())), preferred_element_type=jnp.float32
            )
            scores = scores + bias
            old = m_ref[g]
            new = jnp.maximum(old, jnp.max(scores, 0, keepdims=True))
            weights = jnp.exp2((scores - new) * scale)
            factor = jnp.exp2((old - new) * scale)
            m_ref[g] = new
            l_ref[g] = l_ref[g] * factor + jnp.sum(weights, 0, keepdims=True)
            acc_ref[g] = acc_ref[g] * factor + jnp.dot(
                values, weights.astype(jnp.bfloat16), preferred_element_type=jnp.float32
            )
        return carry

    lax.fori_loop(0, chip - first_chip + 1, one_chip, 0)
    for g in range(heads // together):
        mixed = acc_ref[g] / l_ref[g]
        for i in range(together):
            h = g * together + i
            out_ref[:, h * HEAD_SIZE : (h + 1) * HEAD_SIZE] = mixed[
                :, i * rows : (i + 1) * rows
            ].T.astype(jnp.bfloat16)


def project(count, parts, a_ref, *refs):
    out_ref = refs[count]
    width = out_ref.shape[2]
    weights = jnp.concatenate([w_ref[0] for w_ref in refs[:count]], 1)
    terms = jnp.dot(a_ref[...], weights, preferred_element_type=jnp.float32).astype(jnp.bfloat16)
    for i in range(parts):
        out_ref[i] = terms[:, i * width : (i + 1) * width]


def on_device(query_matrix, key_matrix, value_matrix, doc_ids, out_weight):
    tok_rows = query_matrix.shape[0]
    query_heads = query_matrix.shape[1] // HEAD_SIZE
    members = lax.axis_size("tp")
    ctx_index = lax.axis_index("z") * CORES + lax.axis_index("core")
    weight_blocks = lax.all_gather(out_weight, ("z", "core"), axis=0, tiled=False)
    given_pos = ctx_index * tok_rows + jnp.arange(tok_rows, dtype=jnp.int32)
    info = ctx_index.astype(jnp.int32).reshape(1)
    docs = doc_ids.reshape(-1, tok_rows)
    vmem = pl.BlockSpec(memory_space=pltpu.VMEM)
    smem = pl.BlockSpec(memory_space=pltpu.SMEM)
    hbm = pl.BlockSpec(memory_space=pltpu.HBM)
    small = pltpu.CompilerParams(vmem_limit_bytes=16 * 2**20)
    queries, keys_here, values_here, first = pl.pallas_call(
        functools.partial(prepare, query_heads),
        out_shape=(
            jax.ShapeDtypeStruct((query_heads, tok_rows, HEAD_SIZE), jnp.bfloat16),
            jax.ShapeDtypeStruct(key_matrix.shape, jnp.bfloat16),
            jax.ShapeDtypeStruct(value_matrix.shape[::-1], jnp.bfloat16),
            jax.ShapeDtypeStruct((8, tok_rows), jnp.int32),
        ),
        in_specs=[smem, vmem, vmem] + [hbm] * 4,
        out_specs=(vmem,) * 4,
        scratch_shapes=[
            pltpu.VMEM(x.shape, x.dtype) for x in (query_matrix, key_matrix, value_matrix, docs)
        ]
        + [pltpu.SemaphoreType.DMA((4,))],
        cost_estimate=pl.CostEstimate(flops=10**6, bytes_accessed=10**6, transcendentals=0),
        name="prepare",
    )(info, *rotary_tables(given_pos), query_matrix, key_matrix, value_matrix, docs)
    swap = [(i, CORES - 1 - i) for i in range(CORES)]
    keys_a = lax.all_gather(keys_here, "z", axis=0, tiled=False)
    keys_b = lax.ppermute(keys_a, "core", swap)
    values_a = lax.all_gather(values_here, "z", axis=0, tiled=False)
    values_b = lax.ppermute(values_a, "core", swap)
    together = math.gcd(query_heads, 2)
    sets = query_heads // together
    attention = pl.pallas_call(
        functools.partial(attend, query_heads, together),
        out_shape=jax.ShapeDtypeStruct((tok_rows, query_heads * HEAD_SIZE), jnp.bfloat16),
        in_specs=[smem] + [vmem] * 6,
        out_specs=vmem,
        scratch_shapes=[
            pltpu.VMEM((sets, 1, together * tok_rows), jnp.float32),
            pltpu.VMEM((sets, 1, together * tok_rows), jnp.float32),
            pltpu.VMEM((sets, HEAD_SIZE, together * tok_rows), jnp.float32),
        ],
        cost_estimate=pl.CostEstimate(flops=2 * 10**9, bytes_accessed=3 * 10**6, transcendentals=10**6),
        compiler_params=small,
        name="attend",
    )(info, first, queries, keys_a, keys_b, values_a, values_b)
    blocks, depth, width = weight_blocks.shape
    share = blocks // members
    parts = math.gcd(members, 2)
    count = share * parts
    terms = pl.pallas_call(
        functools.partial(project, count, parts),
        grid=(blocks // count,),
        out_shape=jax.ShapeDtypeStruct((members, tok_rows, share * width), jnp.bfloat16),
        in_specs=[pl.BlockSpec((tok_rows, depth), lambda i: (0, 0))]
        + [
            pl.BlockSpec((1, depth, width), lambda i, j=j: (i * count + j, 0, 0))
            for j in range(count)
        ],
        out_specs=pl.BlockSpec((parts, tok_rows, share * width), lambda i: (i, 0, 0)),
        cost_estimate=pl.CostEstimate(flops=10**9, bytes_accessed=10**7, transcendentals=0),
        name="project",
    )(attention, *[weight_blocks] * count)
    arrived = lax.all_to_all(terms, "tp", split_axis=0, concat_axis=0, tiled=True)
    return arrived.astype(jnp.float32).sum(axis=0).astype(jnp.bfloat16)


def solution(mesh):
    groups, ctx, tp = mesh.devices.shape
    fine = Mesh(mesh.devices.reshape(groups, ctx // CORES, CORES, tp), ("groups", "z", "core", "tp"))
    tokens = ("groups", "z", "core")
    in_specs = (P(tokens, "tp"), P(tokens, "tp"), P(tokens, "tp"), P("groups"), P("tp", ("z", "core")))
    return jax.shard_map(
        on_device, mesh=fine, in_specs=in_specs, out_specs=P(tokens, "tp"), check_vma=False
    )
```

```python
import functools
import math

import jax
import jax.numpy as jnp
from jax import lax
from jax.experimental import pallas as pl
from jax.experimental.pallas import tpu as pltpu
from jax.sharding import Mesh
from jax.sharding import PartitionSpec as P

HEAD_SIZE = 128
CORES = 2
DOCS = 6


rope_base = 1000000.0


def rotary_tables(token_positions):
    half_dim = HEAD_SIZE // 2
    lane = jnp.arange(HEAD_SIZE, dtype=jnp.int32)
    power = -(lane % half_dim).astype(jnp.float32) * (2.0 / HEAD_SIZE)
    angles = token_positions.astype(jnp.float32)[:, None] * jnp.power(jnp.float32(rope_base), power)
    return jnp.cos(angles), jnp.where(lane < half_dim, -1.0, 1.0) * jnp.sin(angles)


def prepare(heads, info, cosine_ref, sine_ref, q_ref, k_ref, v_ref, doc_ref, q_out, k_out, v_out, first_out):
    cosine, sine = cosine_ref[...], sine_ref[...]

    def turned(x):
        x = x.astype(jnp.float32)
        return (x * cosine + pltpu.roll(x, HEAD_SIZE // 2, 1) * sine).astype(jnp.bfloat16)

    k_out[...] = turned(k_ref[...])
    v_out[...] = v_ref[...].astype(jnp.float32).T.astype(jnp.bfloat16)
    for h in range(heads):
        q_out[h] = turned(q_ref[:, h * HEAD_SIZE : (h + 1) * HEAD_SIZE])
    docs, here = doc_ref[...], doc_ref[pl.ds(info[0], 1), :]
    first = jnp.zeros(here.shape, jnp.int32)
    for d in range(1, DOCS):
        before = jnp.sum((docs < d).astype(jnp.int32), keepdims=True)
        first = first + jnp.where(here == d, before, 0)
    first_out[...] = jnp.broadcast_to(first, first_out.shape)


def attend(heads, together, info, first_ref, q_ref, ka_ref, kb_ref, va_ref, vb_ref, out_ref, m_ref, l_ref, acc_ref):
    rows = ka_ref.shape[1]
    ctx = info[0]
    core = lax.rem(ctx, CORES)
    chip = lax.div(ctx, CORES)
    scale = HEAD_SIZE**-0.5 * math.log2(math.e)
    m_ref[...] = jnp.full(m_ref.shape, -1e30, jnp.float32)
    l_ref[...] = jnp.zeros(l_ref.shape, jnp.float32)
    acc_ref[...] = jnp.zeros(acc_ref.shape, jnp.float32)
    width = CORES * rows
    key = lax.broadcasted_iota(jnp.int32, (width, rows), 0)
    given = ctx * rows + lax.broadcasted_iota(jnp.int32, (width, rows), 1)
    mine = key < rows
    first = first_ref[0:1, :]
    first_chip = lax.div(jnp.min(first), width)

    def one_chip(step, carry):
        at = chip - step
        own = (at * CORES + core) * rows
        other = (at * CORES + (1 - core)) * rows - rows
        position = key + jnp.where(mine, own, other)
        bias = jnp.where((position >= first) & (position <= given), 0.0, -1e30)
        bias = jnp.concatenate([bias] * together, 1)
        keys = jnp.concatenate([ka_ref[at], kb_ref[at]], 0)
        values = jnp.concatenate([va_ref[at], vb_ref[at]], 1)
        for g in range(heads // together):
            q = q_ref[g * together : (g + 1) * together].reshape(together * rows, HEAD_SIZE)
            scores = lax.dot_general(
                keys, q, (((1,), (1,)), ((), ())), preferred_element_type=jnp.float32
            )
            scores = scores + bias
            old = m_ref[g]
            new = jnp.maximum(old, jnp.max(scores, 0, keepdims=True))
            weights = jnp.exp2((scores - new) * scale)
            factor = jnp.exp2((old - new) * scale)
            m_ref[g] = new
            l_ref[g] = l_ref[g] * factor + jnp.sum(weights, 0, keepdims=True)
            acc_ref[g] = acc_ref[g] * factor + jnp.dot(
                values, weights.astype(jnp.bfloat16), preferred_element_type=jnp.float32
            )
        return carry

    lax.fori_loop(0, chip - first_chip + 1, one_chip, 0)
    for g in range(heads // together):
        mixed = acc_ref[g] / l_ref[g]
        for i in range(together):
            h = g * together + i
            out_ref[:, h * HEAD_SIZE : (h + 1) * HEAD_SIZE] = mixed[
                :, i * rows : (i + 1) * rows
            ].T.astype(jnp.bfloat16)


def project(count, steps, dests, a_ref, *refs):
    weights = jnp.concatenate([w_ref[0] for w_ref in refs[:count]], 1)
    term = jnp.dot(a_ref[...], weights, preferred_element_type=jnp.float32).astype(jnp.bfloat16)
    for i in range(steps):

        @pl.when(pl.program_id(0) == i)
        def _():
            refs[count + i][...] = term


def projected(attention, weight_blocks, dests, share, name):
    steps = dests.shape[0]
    rows, depth = attention.shape
    width = weight_blocks.shape[2]
    piece = jax.ShapeDtypeStruct((rows, share * width), jnp.bfloat16)
    return pl.pallas_call(
        functools.partial(project, share, steps),
        grid_spec=pltpu.PrefetchScalarGridSpec(
            num_scalar_prefetch=1,
            grid=(steps,),
            in_specs=[pl.BlockSpec((rows, depth), lambda i, d: (0, 0))]
            + [
                pl.BlockSpec((1, depth, width), lambda i, d, j=j: (d[i] * share + j, 0, 0))
                for j in range(share)
            ],
            out_specs=[pl.BlockSpec(piece.shape, lambda i, d: (0, 0))] * steps,
        ),
        out_shape=[piece] * steps,
        cost_estimate=pl.CostEstimate(
            flops=steps * 10**8, bytes_accessed=steps * 10**6, transcendentals=0
        ),
        name=name,
    )(dests, attention, *[weight_blocks] * share)


def total(*refs):
    out_ref = refs[-1]
    value = refs[0][...].astype(jnp.float32)
    for ref in refs[1:-1]:
        value = value + ref[...].astype(jnp.float32)
    out_ref[...] = value.astype(jnp.bfloat16)


def joined(name, params, *pieces):
    vmem = pl.BlockSpec(memory_space=pltpu.VMEM)
    return pl.pallas_call(
        total,
        out_shape=jax.ShapeDtypeStruct(pieces[0].shape, jnp.bfloat16),
        in_specs=[vmem] * len(pieces),
        out_specs=vmem,
        compiler_params=params,
        name=name,
    )(*pieces)


def on_device(query_matrix, key_matrix, value_matrix, doc_ids, out_weight):
    tok_rows = query_matrix.shape[0]
    query_heads = query_matrix.shape[1] // HEAD_SIZE
    members = lax.axis_size("tp")
    ctx_index = lax.axis_index("z") * CORES + lax.axis_index("core")
    weight_blocks = lax.all_gather(out_weight, ("z", "core"), axis=0, tiled=False)
    given_pos = ctx_index * tok_rows + jnp.arange(tok_rows, dtype=jnp.int32)
    info = ctx_index.astype(jnp.int32).reshape(1)
    docs = doc_ids.reshape(-1, tok_rows)
    vmem = pl.BlockSpec(memory_space=pltpu.VMEM)
    smem = pl.BlockSpec(memory_space=pltpu.SMEM)
    small = pltpu.CompilerParams(vmem_limit_bytes=16 * 2**20)
    queries, keys_here, values_here, first = pl.pallas_call(
        functools.partial(prepare, query_heads),
        out_shape=(
            jax.ShapeDtypeStruct((query_heads, tok_rows, HEAD_SIZE), jnp.bfloat16),
            jax.ShapeDtypeStruct(key_matrix.shape, jnp.bfloat16),
            jax.ShapeDtypeStruct(value_matrix.shape[::-1], jnp.bfloat16),
            jax.ShapeDtypeStruct((8, tok_rows), jnp.int32),
        ),
        in_specs=[smem] + [vmem] * 6,
        out_specs=(vmem,) * 4,
        compiler_params=small,
        cost_estimate=pl.CostEstimate(flops=10**6, bytes_accessed=10**6, transcendentals=0),
        name="prepare",
    )(info, *rotary_tables(given_pos), query_matrix, key_matrix, value_matrix, docs)
    swap = [(i, CORES - 1 - i) for i in range(CORES)]
    keys_a = lax.all_gather(keys_here, "z", axis=0, tiled=False)
    keys_b = lax.ppermute(keys_a, "core", swap)
    values_a = lax.all_gather(values_here, "z", axis=0, tiled=False)
    values_b = lax.ppermute(values_a, "core", swap)
    together = 1
    sets = query_heads // together
    attention = pl.pallas_call(
        functools.partial(attend, query_heads, together),
        out_shape=jax.ShapeDtypeStruct((tok_rows, query_heads * HEAD_SIZE), jnp.bfloat16),
        in_specs=[smem] + [vmem] * 6,
        out_specs=vmem,
        scratch_shapes=[
            pltpu.VMEM((sets, 1, together * tok_rows), jnp.float32),
            pltpu.VMEM((sets, 1, together * tok_rows), jnp.float32),
            pltpu.VMEM((sets, HEAD_SIZE, together * tok_rows), jnp.float32),
        ],
        cost_estimate=pl.CostEstimate(flops=2 * 10**9, bytes_accessed=3 * 10**6, transcendentals=10**6),
        compiler_params=small,
        name="attend",
    )(info, first, queries, keys_a, keys_b, values_a, values_b)
    share = weight_blocks.shape[0] // members
    half = members // 2
    my_tp = lax.axis_index("tp")
    near = [k for d in range(half - 1, 0, -1) for k in (d, -d)]

    def shifted(x, by):
        return lax.ppermute(x, "tp", [(i, (i + by) % members) for i in range(members)])

    def of(offsets):
        return (my_tp + members + jnp.array(offsets, jnp.int32)) % members

    (far,) = projected(attention, weight_blocks, of([half]), share, "project_far")
    relayed = shifted(far, -1)
    *pieces, kept = projected(attention, weight_blocks, of(near + [0]), share, "project")
    sends = dict(zip(near, pieces))
    sends[1 - half] = joined("relay", small, sends[1 - half], relayed)
    arrived = [shifted(sends[k], k) for k in near]
    return joined("total", small, kept, *arrived)


def solution(mesh):
    groups, ctx, tp = mesh.devices.shape
    fine = Mesh(mesh.devices.reshape(groups, ctx // CORES, CORES, tp), ("groups", "z", "core", "tp"))
    tokens = ("groups", "z", "core")
    in_specs = (P(tokens, "tp"), P(tokens, "tp"), P(tokens, "tp"), P("groups"), P("tp", ("z", "core")))
    return jax.shard_map(
        on_device, mesh=fine, in_specs=in_specs, out_specs=P(tokens, "tp"), check_vma=False
    )
```

```python
import functools
import math

import jax
import jax.numpy as jnp
from jax import lax
from jax.experimental import pallas as pl
from jax.experimental.pallas import tpu as pltpu
from jax.sharding import Mesh
from jax.sharding import PartitionSpec as P

HEAD_SIZE = 128
CORES = 2
DOCS = 6


rope_base = 1000000.0


def rotary_tables(token_positions):
    half_dim = HEAD_SIZE // 2
    lane = jnp.arange(HEAD_SIZE, dtype=jnp.int32)
    power = -(lane % half_dim).astype(jnp.float32) * (2.0 / HEAD_SIZE)
    angles = token_positions.astype(jnp.float32)[:, None] * jnp.power(jnp.float32(rope_base), power)
    return jnp.cos(angles), jnp.where(lane < half_dim, -1.0, 1.0) * jnp.sin(angles)


def prepare(heads, info, cosine_ref, sine_ref, q_ref, k_ref, v_ref, doc_ref, q_out, k_out, v_out, first_out):
    cosine, sine = cosine_ref[...], sine_ref[...]

    def turned(x):
        x = x.astype(jnp.float32)
        return (x * cosine + pltpu.roll(x, HEAD_SIZE // 2, 1) * sine).astype(jnp.bfloat16)

    k_out[...] = turned(k_ref[...])
    v_out[...] = v_ref[...].astype(jnp.float32).T.astype(jnp.bfloat16)
    for h in range(heads):
        q_out[h] = turned(q_ref[:, h * HEAD_SIZE : (h + 1) * HEAD_SIZE])
    docs, here = doc_ref[...], doc_ref[pl.ds(info[0], 1), :]
    first = jnp.zeros(here.shape, jnp.int32)
    for d in range(1, DOCS):
        before = jnp.sum((docs < d).astype(jnp.int32), keepdims=True)
        first = first + jnp.where(here == d, before, 0)
    first_out[...] = jnp.broadcast_to(first, first_out.shape)


def attend(heads, together, info, first_ref, q_ref, ka_ref, kb_ref, va_ref, vb_ref, out_ref, m_ref, l_ref, acc_ref):
    rows = ka_ref.shape[1]
    ctx = info[0]
    core = lax.rem(ctx, CORES)
    chip = lax.div(ctx, CORES)
    scale = HEAD_SIZE**-0.5 * math.log2(math.e)
    m_ref[...] = jnp.full(m_ref.shape, -1e30, jnp.float32)
    l_ref[...] = jnp.zeros(l_ref.shape, jnp.float32)
    acc_ref[...] = jnp.zeros(acc_ref.shape, jnp.float32)
    width = CORES * rows
    key = lax.broadcasted_iota(jnp.int32, (width, rows), 0)
    given = ctx * rows + lax.broadcasted_iota(jnp.int32, (width, rows), 1)
    mine = key < rows
    first = first_ref[0:1, :]
    first_chip = lax.div(jnp.min(first), width)

    def one_chip(step, carry):
        at = chip - step
        own = (at * CORES + core) * rows
        other = (at * CORES + (1 - core)) * rows - rows
        position = key + jnp.where(mine, own, other)
        bias = jnp.where((position >= first) & (position <= given), 0.0, -1e30)
        bias = jnp.concatenate([bias] * together, 1)
        keys = jnp.concatenate([ka_ref[at], kb_ref[at]], 0)
        values = jnp.concatenate([va_ref[at], vb_ref[at]], 1)
        for g in range(heads // together):
            q = q_ref[g * together : (g + 1) * together].reshape(together * rows, HEAD_SIZE)
            scores = lax.dot_general(
                keys, q, (((1,), (1,)), ((), ())), preferred_element_type=jnp.float32
            )
            scores = scores + bias
            old = m_ref[g]
            new = jnp.maximum(old, jnp.max(scores, 0, keepdims=True))
            weights = jnp.exp2((scores - new) * scale)
            factor = jnp.exp2((old - new) * scale)
            m_ref[g] = new
            l_ref[g] = l_ref[g] * factor + jnp.sum(weights, 0, keepdims=True)
            acc_ref[g] = acc_ref[g] * factor + jnp.dot(
                values, weights.astype(jnp.bfloat16), preferred_element_type=jnp.float32
            )
        return carry

    lax.fori_loop(0, chip - first_chip + 1, one_chip, 0)
    for g in range(heads // together):
        mixed = acc_ref[g] / l_ref[g]
        for i in range(together):
            h = g * together + i
            out_ref[:, h * HEAD_SIZE : (h + 1) * HEAD_SIZE] = mixed[
                :, i * rows : (i + 1) * rows
            ].T.astype(jnp.bfloat16)


def project(share, a_ref, w_hbm, out_ref, w_ref, sems):
    parts = out_ref.shape[0]
    spans = [pl.ds(i * share, share) for i in range(parts)]
    copies = [
        pltpu.make_async_copy(w_hbm.at[at], w_ref.at[at], sems.at[i]) for i, at in enumerate(spans)
    ]
    for copy in copies:
        copy.start()
    for i, copy in enumerate(copies):
        copy.wait()
        weights = jnp.concatenate([w_ref[i * share + j] for j in range(share)], 1)
        out_ref[i] = jnp.dot(a_ref[...], weights, preferred_element_type=jnp.float32).astype(
            jnp.bfloat16
        )


def on_device(query_matrix, key_matrix, value_matrix, doc_ids, out_weight):
    tok_rows = query_matrix.shape[0]
    query_heads = query_matrix.shape[1] // HEAD_SIZE
    members = lax.axis_size("tp")
    ctx_index = lax.axis_index("z") * CORES + lax.axis_index("core")
    weight_blocks = lax.all_gather(out_weight, ("z", "core"), axis=0, tiled=False)
    given_pos = ctx_index * tok_rows + jnp.arange(tok_rows, dtype=jnp.int32)
    info = ctx_index.astype(jnp.int32).reshape(1)
    docs = doc_ids.reshape(-1, tok_rows)
    vmem = pl.BlockSpec(memory_space=pltpu.VMEM)
    smem = pl.BlockSpec(memory_space=pltpu.SMEM)
    small = pltpu.CompilerParams(vmem_limit_bytes=16 * 2**20)
    queries, keys_here, values_here, first = pl.pallas_call(
        functools.partial(prepare, query_heads),
        out_shape=(
            jax.ShapeDtypeStruct((query_heads, tok_rows, HEAD_SIZE), jnp.bfloat16),
            jax.ShapeDtypeStruct(key_matrix.shape, jnp.bfloat16),
            jax.ShapeDtypeStruct(value_matrix.shape[::-1], jnp.bfloat16),
            jax.ShapeDtypeStruct((8, tok_rows), jnp.int32),
        ),
        in_specs=[smem] + [vmem] * 6,
        out_specs=(vmem,) * 4,
        compiler_params=small,
        cost_estimate=pl.CostEstimate(flops=10**6, bytes_accessed=10**6, transcendentals=0),
        name="prepare",
    )(info, *rotary_tables(given_pos), query_matrix, key_matrix, value_matrix, docs)
    swap = [(i, CORES - 1 - i) for i in range(CORES)]
    keys_a = lax.all_gather(keys_here, "z", axis=0, tiled=False)
    keys_b = lax.ppermute(keys_a, "core", swap)
    values_a = lax.all_gather(values_here, "z", axis=0, tiled=False)
    values_b = lax.ppermute(values_a, "core", swap)
    together = 1
    sets = query_heads // together
    attention = pl.pallas_call(
        functools.partial(attend, query_heads, together),
        out_shape=jax.ShapeDtypeStruct((tok_rows, query_heads * HEAD_SIZE), jnp.bfloat16),
        in_specs=[smem] + [vmem] * 6,
        out_specs=vmem,
        scratch_shapes=[
            pltpu.VMEM((sets, 1, together * tok_rows), jnp.float32),
            pltpu.VMEM((sets, 1, together * tok_rows), jnp.float32),
            pltpu.VMEM((sets, HEAD_SIZE, together * tok_rows), jnp.float32),
        ],
        cost_estimate=pl.CostEstimate(flops=2 * 10**9, bytes_accessed=3 * 10**6, transcendentals=10**6),
        compiler_params=small,
        name="attend",
    )(info, first, queries, keys_a, keys_b, values_a, values_b)
    blocks, depth, width = weight_blocks.shape
    share = blocks // members
    terms = pl.pallas_call(
        functools.partial(project, share),
        out_shape=jax.ShapeDtypeStruct((members, tok_rows, share * width), jnp.bfloat16),
        in_specs=[vmem, pl.BlockSpec(memory_space=pl.ANY)],
        out_specs=vmem,
        scratch_shapes=[
            pltpu.VMEM(weight_blocks.shape, jnp.bfloat16),
            pltpu.SemaphoreType.DMA((members,)),
        ],
        compiler_params=pltpu.CompilerParams(vmem_limit_bytes=58 * 2**20),
        cost_estimate=pl.CostEstimate(flops=10**9, bytes_accessed=10**7, transcendentals=0),
        name="project",
    )(attention, weight_blocks)
    arrived = lax.all_to_all(terms, "tp", split_axis=0, concat_axis=0, tiled=True)
    return arrived.astype(jnp.float32).sum(axis=0).astype(jnp.bfloat16)


def solution(mesh):
    groups, ctx, tp = mesh.devices.shape
    fine = Mesh(mesh.devices.reshape(groups, ctx // CORES, CORES, tp), ("groups", "z", "core", "tp"))
    tokens = ("groups", "z", "core")
    in_specs = (P(tokens, "tp"), P(tokens, "tp"), P(tokens, "tp"), P("groups"), P("tp", ("z", "core")))
    return jax.shard_map(
        on_device, mesh=fine, in_specs=in_specs, out_specs=P(tokens, "tp"), check_vma=False
    )
```

```python
import functools
import math

import jax
import jax.numpy as jnp
from jax import lax
from jax.experimental import pallas as pl
from jax.experimental.pallas import tpu as pltpu
from jax.sharding import Mesh
from jax.sharding import PartitionSpec as P

HEAD_SIZE = 128
CORES = 2
REST = 8
DOCS = 6


rope_base = 1000000.0


def rotary_tables(token_positions):
    half_dim = HEAD_SIZE // 2
    lane = jnp.arange(HEAD_SIZE, dtype=jnp.int32)
    power = -(lane % half_dim).astype(jnp.float32) * (2.0 / HEAD_SIZE)
    angles = token_positions.astype(jnp.float32)[:, None] * jnp.power(jnp.float32(rope_base), power)
    return jnp.cos(angles), jnp.where(lane < half_dim, -1.0, 1.0) * jnp.sin(angles)


def prepare(heads, info, cosine_ref, sine_ref, q_ref, k_ref, v_ref, doc_ref, q_out, kv_out, rest_out, first_out):
    cosine, sine = cosine_ref[...], sine_ref[...]

    def turned(x):
        x = x.astype(jnp.float32)
        return (x * cosine + pltpu.roll(x, HEAD_SIZE // 2, 1) * sine).astype(jnp.bfloat16)

    rows = k_ref.shape[0]
    values = v_ref[...].astype(jnp.float32).T
    kept = kv_out.shape[0] - rows
    kv_out[:rows] = turned(k_ref[...])
    kv_out[rows:] = values[:kept].astype(jnp.bfloat16)
    for i in range(rest_out.shape[0]):
        rest_out[i] = values[kept:].astype(jnp.bfloat16)
    for h in range(heads):
        q_out[h] = turned(q_ref[:, h * HEAD_SIZE : (h + 1) * HEAD_SIZE])
    docs, here = doc_ref[...], doc_ref[pl.ds(info[0], 1), :]
    first = jnp.zeros(here.shape, jnp.int32)
    for d in range(1, DOCS):
        before = jnp.sum((docs < d).astype(jnp.int32), keepdims=True)
        first = first + jnp.where(here == d, before, 0)
    first_out[...] = jnp.broadcast_to(first, first_out.shape)


def attend(heads, together, info, first_ref, q_ref, a_ref, b_ref, resta_ref, restb_ref, out_ref, m_ref, l_ref, acc_ref):
    rows = out_ref.shape[0]
    ctx = info[0]
    core = lax.rem(ctx, CORES)
    chip = lax.div(ctx, CORES)
    scale = HEAD_SIZE**-0.5 * math.log2(math.e)
    m_ref[...] = jnp.full(m_ref.shape, -1e30, jnp.float32)
    l_ref[...] = jnp.zeros(l_ref.shape, jnp.float32)
    acc_ref[...] = jnp.zeros(acc_ref.shape, jnp.float32)
    width = CORES * rows
    key = lax.broadcasted_iota(jnp.int32, (width, rows), 0)
    given = ctx * rows + lax.broadcasted_iota(jnp.int32, (width, rows), 1)
    mine = key < rows
    first = first_ref[0:1, :]
    first_chip = lax.div(jnp.min(first), width)

    def one_chip(step, carry):
        at = chip - step
        own = (at * CORES + core) * rows
        other = (at * CORES + (1 - core)) * rows - rows
        position = key + jnp.where(mine, own, other)
        bias = jnp.where((position >= first) & (position <= given), 0.0, -1e30)
        bias = jnp.concatenate([bias] * together, 1)
        keys = jnp.concatenate([a_ref[at, :rows], b_ref[at, :rows]], 0)
        most = jnp.concatenate([a_ref[at, rows:], b_ref[at, rows:]], 1)
        rest = jnp.concatenate([resta_ref[at], restb_ref[at]], 1)
        values = jnp.concatenate([most, rest], 0)
        for g in range(heads // together):
            q = q_ref[g * together : (g + 1) * together].reshape(together * rows, HEAD_SIZE)
            scores = lax.dot_general(
                keys, q, (((1,), (1,)), ((), ())), preferred_element_type=jnp.float32
            )
            scores = scores + bias
            old = m_ref[g]
            new = jnp.maximum(old, jnp.max(scores, 0, keepdims=True))
            weights = jnp.exp2((scores - new) * scale)
            factor = jnp.exp2((old - new) * scale)
            m_ref[g] = new
            l_ref[g] = l_ref[g] * factor + jnp.sum(weights, 0, keepdims=True)
            acc_ref[g] = acc_ref[g] * factor + jnp.dot(
                values, weights.astype(jnp.bfloat16), preferred_element_type=jnp.float32
            )
        return carry

    lax.fori_loop(0, chip - first_chip + 1, one_chip, 0)
    for g in range(heads // together):
        mixed = acc_ref[g] / l_ref[g]
        for i in range(together):
            h = g * together + i
            out_ref[:, h * HEAD_SIZE : (h + 1) * HEAD_SIZE] = mixed[
                :, i * rows : (i + 1) * rows
            ].T.astype(jnp.bfloat16)


def project(share, a_ref, w_hbm, out_ref, w_ref, sems):
    parts = out_ref.shape[0]
    spans = [pl.ds(i * share, share) for i in range(parts)]
    copies = [
        pltpu.make_async_copy(w_hbm.at[at], w_ref.at[at], sems.at[i]) for i, at in enumerate(spans)
    ]
    for copy in copies:
        copy.start()
    for i, copy in enumerate(copies):
        copy.wait()
        weights = jnp.concatenate([w_ref[i * share + j] for j in range(share)], 1)
        out_ref[i] = jnp.dot(a_ref[...], weights, preferred_element_type=jnp.float32).astype(
            jnp.bfloat16
        )


def on_device(query_matrix, key_matrix, value_matrix, doc_ids, out_weight):
    tok_rows = query_matrix.shape[0]
    query_heads = query_matrix.shape[1] // HEAD_SIZE
    members = lax.axis_size("tp")
    ctx_index = lax.axis_index("z") * CORES + lax.axis_index("core")
    weight_blocks = lax.all_gather(out_weight, ("z", "core"), axis=0, tiled=False)
    given_pos = ctx_index * tok_rows + jnp.arange(tok_rows, dtype=jnp.int32)
    info = ctx_index.astype(jnp.int32).reshape(1)
    docs = doc_ids.reshape(-1, tok_rows)
    vmem = pl.BlockSpec(memory_space=pltpu.VMEM)
    smem = pl.BlockSpec(memory_space=pltpu.SMEM)
    small = pltpu.CompilerParams(vmem_limit_bytes=16 * 2**20)
    chips = lax.axis_size("z")
    queries, here, rest_here, first = pl.pallas_call(
        functools.partial(prepare, query_heads),
        out_shape=(
            jax.ShapeDtypeStruct((query_heads, tok_rows, HEAD_SIZE), jnp.bfloat16),
            jax.ShapeDtypeStruct((tok_rows + HEAD_SIZE - REST, HEAD_SIZE), jnp.bfloat16),
            jax.ShapeDtypeStruct((chips, REST, tok_rows), jnp.bfloat16),
            jax.ShapeDtypeStruct((8, tok_rows), jnp.int32),
        ),
        in_specs=[smem] + [vmem] * 6,
        out_specs=(vmem,) * 4,
        compiler_params=small,
        cost_estimate=pl.CostEstimate(flops=10**6, bytes_accessed=10**6, transcendentals=0),
        name="prepare",
    )(info, *rotary_tables(given_pos), query_matrix, key_matrix, value_matrix, docs)
    swap = [(i, CORES - 1 - i) for i in range(CORES)]
    most_a = lax.all_gather(here, "z", axis=0, tiled=False)
    most_b = lax.ppermute(most_a, "core", swap)
    rest_a = lax.all_to_all(rest_here, "z", split_axis=0, concat_axis=0, tiled=True)
    rest_b = lax.ppermute(rest_a, "core", swap)
    together = 1
    sets = query_heads // together
    attention = pl.pallas_call(
        functools.partial(attend, query_heads, together),
        out_shape=jax.ShapeDtypeStruct((tok_rows, query_heads * HEAD_SIZE), jnp.bfloat16),
        in_specs=[smem] + [vmem] * 6,
        out_specs=vmem,
        scratch_shapes=[
            pltpu.VMEM((sets, 1, together * tok_rows), jnp.float32),
            pltpu.VMEM((sets, 1, together * tok_rows), jnp.float32),
            pltpu.VMEM((sets, HEAD_SIZE, together * tok_rows), jnp.float32),
        ],
        cost_estimate=pl.CostEstimate(flops=2 * 10**9, bytes_accessed=3 * 10**6, transcendentals=10**6),
        compiler_params=small,
        name="attend",
    )(info, first, queries, most_a, most_b, rest_a, rest_b)
    blocks, depth, width = weight_blocks.shape
    share = blocks // members
    terms = pl.pallas_call(
        functools.partial(project, share),
        out_shape=jax.ShapeDtypeStruct((members, tok_rows, share * width), jnp.bfloat16),
        in_specs=[vmem, pl.BlockSpec(memory_space=pl.ANY)],
        out_specs=vmem,
        scratch_shapes=[
            pltpu.VMEM(weight_blocks.shape, jnp.bfloat16),
            pltpu.SemaphoreType.DMA((members,)),
        ],
        compiler_params=pltpu.CompilerParams(vmem_limit_bytes=58 * 2**20),
        cost_estimate=pl.CostEstimate(flops=10**9, bytes_accessed=10**7, transcendentals=0),
        name="project",
    )(attention, weight_blocks)
    arrived = lax.all_to_all(terms, "tp", split_axis=0, concat_axis=0, tiled=True)
    return arrived.astype(jnp.float32).sum(axis=0).astype(jnp.bfloat16)


def solution(mesh):
    groups, ctx, tp = mesh.devices.shape
    fine = Mesh(mesh.devices.reshape(groups, ctx // CORES, CORES, tp), ("groups", "z", "core", "tp"))
    tokens = ("groups", "z", "core")
    in_specs = (P(tokens, "tp"), P(tokens, "tp"), P(tokens, "tp"), P("groups"), P("tp", ("z", "core")))
    return jax.shard_map(
        on_device, mesh=fine, in_specs=in_specs, out_specs=P(tokens, "tp"), check_vma=False
    )
```

```python
import functools
import math

import jax
import jax.numpy as jnp
from jax import lax
from jax.experimental import pallas as pl
from jax.experimental.pallas import tpu as pltpu
from jax.sharding import Mesh
from jax.sharding import PartitionSpec as P

HEAD_SIZE = 128
CORES = 2
REST = 8
DOCS = 6


rope_base = 1000000.0


def rotary_tables(token_positions):
    half_dim = HEAD_SIZE // 2
    lane = jnp.arange(HEAD_SIZE, dtype=jnp.int32)
    power = -(lane % half_dim).astype(jnp.float32) * (2.0 / HEAD_SIZE)
    angles = token_positions.astype(jnp.float32)[:, None] * jnp.power(jnp.float32(rope_base), power)
    return jnp.cos(angles), jnp.where(lane < half_dim, -1.0, 1.0) * jnp.sin(angles)


def prepare(heads, info, cosine_ref, sine_ref, q_ref, k_ref, v_ref, doc_ref, q_out, kv_out, rest_out, first_out):
    cosine, sine = cosine_ref[...], sine_ref[...]

    def turned(x):
        x = x.astype(jnp.float32)
        return (x * cosine + pltpu.roll(x, HEAD_SIZE // 2, 1) * sine).astype(jnp.bfloat16)

    rows = k_ref.shape[0]
    values = v_ref[...].astype(jnp.float32).T
    kept = kv_out.shape[0] - rows
    kv_out[:rows] = turned(k_ref[...])
    kv_out[rows:] = values[:kept].astype(jnp.bfloat16)
    for i in range(rest_out.shape[0]):
        rest_out[i] = values[kept:].astype(jnp.bfloat16)
    for h in range(heads):
        q_out[h] = turned(q_ref[:, h * HEAD_SIZE : (h + 1) * HEAD_SIZE])
    docs, here = doc_ref[...], doc_ref[pl.ds(info[0], 1), :]
    first = jnp.zeros(here.shape, jnp.int32)
    for d in range(1, DOCS):
        before = jnp.sum((docs < d).astype(jnp.int32), keepdims=True)
        first = first + jnp.where(here == d, before, 0)
    first_out[...] = jnp.broadcast_to(first, first_out.shape)


def attend(heads, together, info, first_ref, q_ref, a_ref, b_ref, resta_ref, restb_ref, out_ref, m_ref, l_ref, acc_ref):
    rows = out_ref.shape[0]
    ctx = info[0]
    core = lax.rem(ctx, CORES)
    chip = lax.div(ctx, CORES)
    scale = HEAD_SIZE**-0.5 * math.log2(math.e)
    m_ref[...] = jnp.full(m_ref.shape, -1e30, jnp.float32)
    l_ref[...] = jnp.zeros(l_ref.shape, jnp.float32)
    acc_ref[...] = jnp.zeros(acc_ref.shape, jnp.float32)
    width = CORES * rows
    key = lax.broadcasted_iota(jnp.int32, (width, rows), 0)
    given = ctx * rows + lax.broadcasted_iota(jnp.int32, (width, rows), 1)
    mine = key < rows
    first = first_ref[0:1, :]
    first_chip = lax.div(jnp.min(first), width)

    def one_chip(step, carry):
        at = chip - step
        own = (at * CORES + core) * rows
        other = (at * CORES + (1 - core)) * rows - rows
        position = key + jnp.where(mine, own, other)
        bias = jnp.where((position >= first) & (position <= given), 0.0, -1e30)
        bias = jnp.concatenate([bias] * together, 1)
        keys = jnp.concatenate([a_ref[at, :rows], b_ref[at, :rows]], 0)
        most = jnp.concatenate([a_ref[at, rows:], b_ref[at, rows:]], 1)
        rest = jnp.concatenate([resta_ref[at], restb_ref[at]], 1)
        values = jnp.concatenate([most, rest], 0)
        for g in range(heads // together):
            q = q_ref[g * together : (g + 1) * together].reshape(together * rows, HEAD_SIZE)
            scores = lax.dot_general(
                keys, q, (((1,), (1,)), ((), ())), preferred_element_type=jnp.float32
            )
            scores = scores + bias
            old = m_ref[g]
            new = jnp.maximum(old, jnp.max(scores, 0, keepdims=True))
            weights = jnp.exp2((scores - new) * scale)
            factor = jnp.exp2((old - new) * scale)
            m_ref[g] = new
            l_ref[g] = l_ref[g] * factor + jnp.sum(weights, 0, keepdims=True)
            acc_ref[g] = acc_ref[g] * factor + jnp.dot(
                values, weights.astype(jnp.bfloat16), preferred_element_type=jnp.float32
            )
        return carry

    lax.fori_loop(0, chip - first_chip + 1, one_chip, 0)
    for g in range(heads // together):
        mixed = acc_ref[g] / l_ref[g]
        for i in range(together):
            h = g * together + i
            out_ref[:, h * HEAD_SIZE : (h + 1) * HEAD_SIZE] = mixed[
                :, i * rows : (i + 1) * rows
            ].T.astype(jnp.bfloat16)


def project(share, own_ref, other_ref, w_hbm, out_ref, w_ref, sems):
    parts = out_ref.shape[0]
    spans = [pl.ds(i * share, share) for i in range(parts)]
    copies = [
        pltpu.make_async_copy(w_hbm.at[at], w_ref.at[at], sems.at[i]) for i, at in enumerate(spans)
    ]
    for copy in copies:
        copy.start()
    both = jnp.concatenate([own_ref[...], other_ref[...]], 0)
    for i, copy in enumerate(copies):
        copy.wait()
        weights = jnp.concatenate([w_ref[i * share + j] for j in range(share)], 1)
        out_ref[i] = jnp.dot(both, weights, preferred_element_type=jnp.float32).astype(
            jnp.bfloat16
        )


def total(terms_ref, kept_ref, sent_ref):
    rows = kept_ref.shape[0]
    for i, out_ref in enumerate((kept_ref, sent_ref)):
        at = slice(i * rows, (i + 1) * rows)
        out_ref[...] = jnp.sum(terms_ref[:, at].astype(jnp.float32), 0).astype(jnp.bfloat16)


def weave(count, core, kept_ref, given_ref, out_ref):
    width = kept_ref.shape[1] // count
    even = core[0] == 0
    for j in range(count):
        kept, given = (r[:, j * width : (j + 1) * width] for r in (kept_ref, given_ref))
        at = j * CORES * width
        out_ref[:, at : at + width] = jnp.where(even, kept, given)
        out_ref[:, at + width : at + CORES * width] = jnp.where(even, given, kept)


def on_device(query_matrix, key_matrix, value_matrix, doc_ids, out_weight):
    tok_rows = query_matrix.shape[0]
    query_heads = query_matrix.shape[1] // HEAD_SIZE
    members = lax.axis_size("tp")
    core = lax.axis_index("core")
    ctx_index = lax.axis_index("z") * CORES + core
    weight_blocks = lax.all_gather(out_weight, "z", axis=0, tiled=False)
    given_pos = ctx_index * tok_rows + jnp.arange(tok_rows, dtype=jnp.int32)
    info = ctx_index.astype(jnp.int32).reshape(1)
    docs = doc_ids.reshape(-1, tok_rows)
    vmem = pl.BlockSpec(memory_space=pltpu.VMEM)
    smem = pl.BlockSpec(memory_space=pltpu.SMEM)
    small = pltpu.CompilerParams(vmem_limit_bytes=16 * 2**20)
    chips = lax.axis_size("z")
    queries, here, rest_here, first = pl.pallas_call(
        functools.partial(prepare, query_heads),
        out_shape=(
            jax.ShapeDtypeStruct((query_heads, tok_rows, HEAD_SIZE), jnp.bfloat16),
            jax.ShapeDtypeStruct((tok_rows + HEAD_SIZE - REST, HEAD_SIZE), jnp.bfloat16),
            jax.ShapeDtypeStruct((chips, REST, tok_rows), jnp.bfloat16),
            jax.ShapeDtypeStruct((8, tok_rows), jnp.int32),
        ),
        in_specs=[smem] + [vmem] * 6,
        out_specs=(vmem,) * 4,
        compiler_params=small,
        cost_estimate=pl.CostEstimate(flops=10**6, bytes_accessed=10**6, transcendentals=0),
        name="prepare",
    )(info, *rotary_tables(given_pos), query_matrix, key_matrix, value_matrix, docs)
    swap = [(i, CORES - 1 - i) for i in range(CORES)]
    most_a = lax.all_gather(here, "z", axis=0, tiled=False)
    most_b = lax.ppermute(most_a, "core", swap)
    rest_a = lax.all_to_all(rest_here, "z", split_axis=0, concat_axis=0, tiled=True)
    rest_b = lax.ppermute(rest_a, "core", swap)
    together = 1
    sets = query_heads // together
    attention = pl.pallas_call(
        functools.partial(attend, query_heads, together),
        out_shape=jax.ShapeDtypeStruct((tok_rows, query_heads * HEAD_SIZE), jnp.bfloat16),
        in_specs=[smem] + [vmem] * 6,
        out_specs=vmem,
        scratch_shapes=[
            pltpu.VMEM((sets, 1, together * tok_rows), jnp.float32),
            pltpu.VMEM((sets, 1, together * tok_rows), jnp.float32),
            pltpu.VMEM((sets, HEAD_SIZE, together * tok_rows), jnp.float32),
        ],
        cost_estimate=pl.CostEstimate(flops=2 * 10**9, bytes_accessed=3 * 10**6, transcendentals=10**6),
        compiler_params=small,
        name="attend",
    )(info, first, queries, most_a, most_b, rest_a, rest_b)
    attention_other = lax.ppermute(attention, "core", swap)
    blocks, depth, width = weight_blocks.shape
    share = blocks // members
    terms = pl.pallas_call(
        functools.partial(project, share),
        out_shape=jax.ShapeDtypeStruct((members, CORES * tok_rows, share * width), jnp.bfloat16),
        in_specs=[vmem, vmem, pl.BlockSpec(memory_space=pltpu.HBM)],
        out_specs=vmem,
        scratch_shapes=[
            pltpu.VMEM(weight_blocks.shape, jnp.bfloat16),
            pltpu.SemaphoreType.DMA((members,)),
        ],
        compiler_params=pltpu.CompilerParams(vmem_limit_bytes=59 * 2**20),
        cost_estimate=pl.CostEstimate(flops=10**9, bytes_accessed=10**7, transcendentals=0),
        name="project",
    )(attention, attention_other, weight_blocks)
    arrived = lax.all_to_all(terms, "tp", split_axis=0, concat_axis=0, tiled=True)
    half = jax.ShapeDtypeStruct((tok_rows, share * width), jnp.bfloat16)
    kept, sent = pl.pallas_call(
        total,
        out_shape=(half, half),
        in_specs=[vmem],
        out_specs=(vmem, vmem),
        compiler_params=small,
        name="total",
    )(arrived)
    given = lax.ppermute(sent, "core", swap)
    return pl.pallas_call(
        functools.partial(weave, share),
        out_shape=jax.ShapeDtypeStruct((tok_rows, share * CORES * width), jnp.bfloat16),
        in_specs=[pl.BlockSpec(memory_space=pltpu.SMEM), vmem, vmem],
        out_specs=vmem,
        compiler_params=small,
        name="weave",
    )(core.astype(jnp.int32).reshape(1), kept, given)


def solution(mesh):
    groups, ctx, tp = mesh.devices.shape
    fine = Mesh(mesh.devices.reshape(groups, ctx // CORES, CORES, tp), ("groups", "z", "core", "tp"))
    tokens = ("groups", "z", "core")
    in_specs = (P(tokens, "tp"), P(tokens, "tp"), P(tokens, "tp"), P("groups"), P("tp", ("z", "core")))
    return jax.shard_map(
        on_device, mesh=fine, in_specs=in_specs, out_specs=P(tokens, "tp"), check_vma=False
    )
```

```python
import functools
import math

import jax
import jax.numpy as jnp
from jax import lax
from jax.experimental import pallas as pl
from jax.experimental.pallas import tpu as pltpu
from jax.sharding import Mesh
from jax.sharding import PartitionSpec as P

HEAD_SIZE = 128
CORES = 2
REST = 8
DOCS = 6


rope_base = 1000000.0


def rotary_tables(token_positions):
    half_dim = HEAD_SIZE // 2
    lane = jnp.arange(HEAD_SIZE, dtype=jnp.int32)
    power = -(lane % half_dim).astype(jnp.float32) * (2.0 / HEAD_SIZE)
    angles = token_positions.astype(jnp.float32)[:, None] * jnp.power(jnp.float32(rope_base), power)
    return jnp.cos(angles), jnp.where(lane < half_dim, -1.0, 1.0) * jnp.sin(angles)


def prepare(heads, info, cosine_ref, sine_ref, q_ref, k_ref, v_ref, doc_ref, q_out, kv_out, rest_out, first_out):
    cosine, sine = cosine_ref[...], sine_ref[...]

    def turned(x):
        x = x.astype(jnp.float32)
        return (x * cosine + pltpu.roll(x, HEAD_SIZE // 2, 1) * sine).astype(jnp.bfloat16)

    rows = k_ref.shape[0]
    values = v_ref[...].astype(jnp.float32).T
    kept = kv_out.shape[0] - rows
    kv_out[:rows] = turned(k_ref[...])
    kv_out[rows:] = values[:kept].astype(jnp.bfloat16)
    for i in range(rest_out.shape[0]):
        rest_out[i] = values[kept:].astype(jnp.bfloat16)
    for h in range(heads):
        q_out[h] = turned(q_ref[:, h * HEAD_SIZE : (h + 1) * HEAD_SIZE])
    docs, here = doc_ref[...], doc_ref[pl.ds(info[0], 1), :]
    first = jnp.zeros(here.shape, jnp.int32)
    for d in range(1, DOCS):
        before = jnp.sum((docs < d).astype(jnp.int32), keepdims=True)
        first = first + jnp.where(here == d, before, 0)
    first_out[...] = jnp.broadcast_to(first, first_out.shape)


def attend(heads, together, info, first_ref, q_ref, a_ref, b_ref, resta_ref, restb_ref, out_ref, m_ref, l_ref, acc_ref):
    rows = out_ref.shape[0]
    ctx = info[0]
    core = lax.rem(ctx, CORES)
    chip = lax.div(ctx, CORES)
    scale = HEAD_SIZE**-0.5 * math.log2(math.e)
    m_ref[...] = jnp.full(m_ref.shape, -1e30, jnp.float32)
    l_ref[...] = jnp.zeros(l_ref.shape, jnp.float32)
    acc_ref[...] = jnp.zeros(acc_ref.shape, jnp.float32)
    width = CORES * rows
    key = lax.broadcasted_iota(jnp.int32, (width, rows), 0)
    given = ctx * rows + lax.broadcasted_iota(jnp.int32, (width, rows), 1)
    mine = key < rows
    first = first_ref[0:1, :]
    first_chip = lax.div(jnp.min(first), width)

    def one_chip(step, carry):
        at = chip - step
        own = (at * CORES + core) * rows
        other = (at * CORES + (1 - core)) * rows - rows
        position = key + jnp.where(mine, own, other)
        bias = jnp.where((position >= first) & (position <= given), 0.0, -1e30)
        bias = jnp.concatenate([bias] * together, 1)
        keys = jnp.concatenate([a_ref[at, :rows], b_ref[at, :rows]], 0)
        most = jnp.concatenate([a_ref[at, rows:], b_ref[at, rows:]], 1)
        rest = jnp.concatenate([resta_ref[at], restb_ref[at]], 1)
        values = jnp.concatenate([most, rest], 0)
        for g in range(heads // together):
            q = q_ref[g * together : (g + 1) * together].reshape(together * rows, HEAD_SIZE)
            scores = lax.dot_general(
                keys, q, (((1,), (1,)), ((), ())), preferred_element_type=jnp.float32
            )
            scores = scores + bias
            old = m_ref[g]
            new = jnp.maximum(old, jnp.max(scores, 0, keepdims=True))
            weights = jnp.exp2((scores - new) * scale)
            factor = jnp.exp2((old - new) * scale)
            m_ref[g] = new
            l_ref[g] = l_ref[g] * factor + jnp.sum(weights, 0, keepdims=True)
            acc_ref[g] = acc_ref[g] * factor + jnp.dot(
                values, weights.astype(jnp.bfloat16), preferred_element_type=jnp.float32
            )
        return carry

    lax.fori_loop(0, chip - first_chip + 1, one_chip, 0)
    for g in range(heads // together):
        mixed = acc_ref[g] / l_ref[g]
        for i in range(together):
            h = g * together + i
            out_ref[:, h * HEAD_SIZE : (h + 1) * HEAD_SIZE] = mixed[
                :, i * rows : (i + 1) * rows
            ].T.astype(jnp.bfloat16)


def project(share, own_ref, other_ref, w_hbm, out_ref, w_ref, sems):
    parts = out_ref.shape[0]
    spans = [pl.ds(i * share, share) for i in range(parts)]
    copies = [
        pltpu.make_async_copy(w_hbm.at[at], w_ref.at[at], sems.at[i]) for i, at in enumerate(spans)
    ]
    for copy in copies:
        copy.start()
    both = jnp.concatenate([own_ref[...], other_ref[...]], 0)
    width = out_ref.shape[2]
    group = math.gcd(parts, 2)
    for g in range(0, parts, group):
        for copy in copies[g : g + group]:
            copy.wait()
        blocks = range(g * share, (g + group) * share)
        weights = jnp.concatenate([w_ref[j] for j in blocks], 1)
        terms = jnp.dot(both, weights, preferred_element_type=jnp.float32).astype(jnp.bfloat16)
        for i in range(group):
            out_ref[g + i] = terms[:, i * width : (i + 1) * width]


def total(terms_ref, kept_ref, sent_ref):
    rows = kept_ref.shape[0]
    for i, out_ref in enumerate((kept_ref, sent_ref)):
        at = slice(i * rows, (i + 1) * rows)
        out_ref[...] = jnp.sum(terms_ref[:, at].astype(jnp.float32), 0).astype(jnp.bfloat16)


def weave(count, core, kept_ref, given_ref, out_ref):
    width = kept_ref.shape[1] // count
    even = core[0] == 0
    for j in range(count):
        kept, given = (r[:, j * width : (j + 1) * width] for r in (kept_ref, given_ref))
        at = j * CORES * width
        out_ref[:, at : at + width] = jnp.where(even, kept, given)
        out_ref[:, at + width : at + CORES * width] = jnp.where(even, given, kept)


def on_device(query_matrix, key_matrix, value_matrix, doc_ids, out_weight):
    tok_rows = query_matrix.shape[0]
    query_heads = query_matrix.shape[1] // HEAD_SIZE
    members = lax.axis_size("tp")
    core = lax.axis_index("core")
    ctx_index = lax.axis_index("z") * CORES + core
    weight_blocks = lax.all_gather(out_weight, "z", axis=0, tiled=False)
    given_pos = ctx_index * tok_rows + jnp.arange(tok_rows, dtype=jnp.int32)
    info = ctx_index.astype(jnp.int32).reshape(1)
    docs = doc_ids.reshape(-1, tok_rows)
    vmem = pl.BlockSpec(memory_space=pltpu.VMEM)
    smem = pl.BlockSpec(memory_space=pltpu.SMEM)
    small = pltpu.CompilerParams(vmem_limit_bytes=16 * 2**20)
    chips = lax.axis_size("z")
    queries, here, rest_here, first = pl.pallas_call(
        functools.partial(prepare, query_heads),
        out_shape=(
            jax.ShapeDtypeStruct((query_heads, tok_rows, HEAD_SIZE), jnp.bfloat16),
            jax.ShapeDtypeStruct((tok_rows + HEAD_SIZE - REST, HEAD_SIZE), jnp.bfloat16),
            jax.ShapeDtypeStruct((chips, REST, tok_rows), jnp.bfloat16),
            jax.ShapeDtypeStruct((8, tok_rows), jnp.int32),
        ),
        in_specs=[smem] + [vmem] * 6,
        out_specs=(vmem,) * 4,
        compiler_params=small,
        cost_estimate=pl.CostEstimate(flops=10**6, bytes_accessed=10**6, transcendentals=0),
        name="prepare",
    )(info, *rotary_tables(given_pos), query_matrix, key_matrix, value_matrix, docs)
    swap = [(i, CORES - 1 - i) for i in range(CORES)]
    most_a = lax.all_gather(here, "z", axis=0, tiled=False)
    most_b = lax.ppermute(most_a, "core", swap)
    rest_a = lax.all_to_all(rest_here, "z", split_axis=0, concat_axis=0, tiled=True)
    rest_b = lax.ppermute(rest_a, "core", swap)
    together = 1
    sets = query_heads // together
    attention = pl.pallas_call(
        functools.partial(attend, query_heads, together),
        out_shape=jax.ShapeDtypeStruct((tok_rows, query_heads * HEAD_SIZE), jnp.bfloat16),
        in_specs=[smem] + [vmem] * 6,
        out_specs=vmem,
        scratch_shapes=[
            pltpu.VMEM((sets, 1, together * tok_rows), jnp.float32),
            pltpu.VMEM((sets, 1, together * tok_rows), jnp.float32),
            pltpu.VMEM((sets, HEAD_SIZE, together * tok_rows), jnp.float32),
        ],
        cost_estimate=pl.CostEstimate(flops=2 * 10**9, bytes_accessed=3 * 10**6, transcendentals=10**6),
        compiler_params=small,
        name="attend",
    )(info, first, queries, most_a, most_b, rest_a, rest_b)
    attention_other = lax.ppermute(attention, "core", swap)
    blocks, depth, width = weight_blocks.shape
    share = blocks // members
    terms = pl.pallas_call(
        functools.partial(project, share),
        out_shape=jax.ShapeDtypeStruct((members, CORES * tok_rows, share * width), jnp.bfloat16),
        in_specs=[vmem, vmem, pl.BlockSpec(memory_space=pltpu.HBM)],
        out_specs=vmem,
        scratch_shapes=[
            pltpu.VMEM(weight_blocks.shape, jnp.bfloat16),
            pltpu.SemaphoreType.DMA((members,)),
        ],
        compiler_params=pltpu.CompilerParams(vmem_limit_bytes=59 * 2**20),
        cost_estimate=pl.CostEstimate(flops=10**9, bytes_accessed=10**7, transcendentals=0),
        name="project",
    )(attention, attention_other, weight_blocks)
    arrived = lax.all_to_all(terms, "tp", split_axis=0, concat_axis=0, tiled=True)
    half = jax.ShapeDtypeStruct((tok_rows, share * width), jnp.bfloat16)
    kept, sent = pl.pallas_call(
        total,
        out_shape=(half, half),
        in_specs=[vmem],
        out_specs=(vmem, vmem),
        compiler_params=small,
        name="total",
    )(arrived)
    given = lax.ppermute(sent, "core", swap)
    return pl.pallas_call(
        functools.partial(weave, share),
        out_shape=jax.ShapeDtypeStruct((tok_rows, share * CORES * width), jnp.bfloat16),
        in_specs=[pl.BlockSpec(memory_space=pltpu.SMEM), vmem, vmem],
        out_specs=vmem,
        compiler_params=small,
        name="weave",
    )(core.astype(jnp.int32).reshape(1), kept, given)


def solution(mesh):
    groups, ctx, tp = mesh.devices.shape
    fine = Mesh(mesh.devices.reshape(groups, ctx // CORES, CORES, tp), ("groups", "z", "core", "tp"))
    tokens = ("groups", "z", "core")
    in_specs = (P(tokens, "tp"), P(tokens, "tp"), P(tokens, "tp"), P("groups"), P("tp", ("z", "core")))
    return jax.shard_map(
        on_device, mesh=fine, in_specs=in_specs, out_specs=P(tokens, "tp"), check_vma=False
    )
```

```python
import functools
import math

import jax
import jax.numpy as jnp
from jax import lax
from jax.experimental import pallas as pl
from jax.experimental.pallas import tpu as pltpu
from jax.sharding import Mesh
from jax.sharding import PartitionSpec as P

HEAD_SIZE = 128
CORES = 2
REST = 8
DOCS = 6


rope_base = 1000000.0


def rotary_tables(token_positions):
    half_dim = HEAD_SIZE // 2
    lane = jnp.arange(HEAD_SIZE, dtype=jnp.int32)
    power = -(lane % half_dim).astype(jnp.float32) * (2.0 / HEAD_SIZE)
    angles = token_positions.astype(jnp.float32)[:, None] * jnp.power(jnp.float32(rope_base), power)
    return jnp.cos(angles), jnp.where(lane < half_dim, -1.0, 1.0) * jnp.sin(angles)


def prepare(heads, info, cosine_ref, sine_ref, q_ref, k_ref, v_ref, doc_ref, q_out, kv_out, rest_out, first_out):
    cosine, sine = cosine_ref[...], sine_ref[...]

    def turned(x):
        x = x.astype(jnp.float32)
        return (x * cosine + pltpu.roll(x, HEAD_SIZE // 2, 1) * sine).astype(jnp.bfloat16)

    rows = k_ref.shape[0]
    values = v_ref[...].astype(jnp.float32).T
    kept = kv_out.shape[0] - rows
    kv_out[:rows] = turned(k_ref[...])
    kv_out[rows:] = values[:kept].astype(jnp.bfloat16)
    for i in range(rest_out.shape[0]):
        rest_out[i] = values[kept:].astype(jnp.bfloat16)
    for h in range(heads):
        q_out[h] = turned(q_ref[:, h * HEAD_SIZE : (h + 1) * HEAD_SIZE])
    docs, here = doc_ref[...], doc_ref[pl.ds(info[0], 1), :]
    first = jnp.zeros(here.shape, jnp.int32)
    for d in range(1, DOCS):
        before = jnp.sum((docs < d).astype(jnp.int32), keepdims=True)
        first = first + jnp.where(here == d, before, 0)
    first_out[...] = jnp.broadcast_to(first, first_out.shape)


def attend(heads, together, info, first_ref, q_ref, a_ref, b_ref, resta_ref, restb_ref, out_ref, m_ref, l_ref, acc_ref):
    rows = out_ref.shape[0]
    ctx = info[0]
    core = lax.rem(ctx, CORES)
    chip = lax.div(ctx, CORES)
    scale = HEAD_SIZE**-0.5 * math.log2(math.e)
    m_ref[...] = jnp.full(m_ref.shape, -1e30, jnp.float32)
    l_ref[...] = jnp.zeros(l_ref.shape, jnp.float32)
    acc_ref[...] = jnp.zeros(acc_ref.shape, jnp.float32)
    width = CORES * rows
    key = lax.broadcasted_iota(jnp.int32, (width, rows), 0)
    given = ctx * rows + lax.broadcasted_iota(jnp.int32, (width, rows), 1)
    mine = key < rows
    first = first_ref[0:1, :]
    first_chip = lax.div(jnp.min(first), width)

    def one_chip(step, carry):
        at = chip - step
        own = (at * CORES + core) * rows
        other = (at * CORES + (1 - core)) * rows - rows
        position = key + jnp.where(mine, own, other)
        bias = jnp.where((position >= first) & (position <= given), 0.0, -1e30)
        bias = jnp.concatenate([bias] * together, 1)
        keys = jnp.concatenate([a_ref[at, :rows], b_ref[at, :rows]], 0)
        most = jnp.concatenate([a_ref[at, rows:], b_ref[at, rows:]], 1)
        rest = jnp.concatenate([resta_ref[at], restb_ref[at]], 1)
        values = jnp.concatenate([most, rest], 0)
        for g in range(heads // together):
            q = q_ref[g * together : (g + 1) * together].reshape(together * rows, HEAD_SIZE)
            scores = lax.dot_general(
                keys, q, (((1,), (1,)), ((), ())), preferred_element_type=jnp.float32
            )
            scores = scores + bias
            old = m_ref[g]
            new = jnp.maximum(old, jnp.max(scores, 0, keepdims=True))
            weights = jnp.exp2((scores - new) * scale)
            factor = jnp.exp2((old - new) * scale)
            m_ref[g] = new
            l_ref[g] = l_ref[g] * factor + jnp.sum(weights, 0, keepdims=True)
            acc_ref[g] = acc_ref[g] * factor + jnp.dot(
                values, weights.astype(jnp.bfloat16), preferred_element_type=jnp.float32
            )
        return carry

    lax.fori_loop(0, chip - first_chip + 1, one_chip, 0)
    for g in range(heads // together):
        mixed = acc_ref[g] / l_ref[g]
        for i in range(together):
            h = g * together + i
            out_ref[:, h * HEAD_SIZE : (h + 1) * HEAD_SIZE] = mixed[
                :, i * rows : (i + 1) * rows
            ].T.astype(jnp.bfloat16)


def project(share, own_ref, other_ref, w_hbm, out_ref, w_ref, sems):
    parts = out_ref.shape[0]
    spans = [pl.ds(i * share, share) for i in range(parts)]
    copies = [
        pltpu.make_async_copy(w_hbm.at[at], w_ref.at[at], sems.at[i]) for i, at in enumerate(spans)
    ]
    for copy in copies:
        copy.start()
    both = jnp.concatenate([own_ref[...], other_ref[...]], 0)
    width = out_ref.shape[2]
    group = math.gcd(parts, 4)
    for g in range(0, parts, group):
        for copy in copies[g : g + group]:
            copy.wait()
        blocks = range(g * share, (g + group) * share)
        weights = jnp.concatenate([w_ref[j] for j in blocks], 1)
        terms = jnp.dot(both, weights, preferred_element_type=jnp.float32).astype(jnp.bfloat16)
        for i in range(group):
            out_ref[g + i] = terms[:, i * width : (i + 1) * width]


def total(terms_ref, kept_ref, sent_ref):
    rows = kept_ref.shape[0]
    for i, out_ref in enumerate((kept_ref, sent_ref)):
        at = slice(i * rows, (i + 1) * rows)
        out_ref[...] = jnp.sum(terms_ref[:, at].astype(jnp.float32), 0).astype(jnp.bfloat16)


def weave(count, core, kept_ref, given_ref, out_ref):
    width = kept_ref.shape[1] // count
    even = core[0] == 0
    for j in range(count):
        kept, given = (r[:, j * width : (j + 1) * width] for r in (kept_ref, given_ref))
        at = j * CORES * width
        out_ref[:, at : at + width] = jnp.where(even, kept, given)
        out_ref[:, at + width : at + CORES * width] = jnp.where(even, given, kept)


def on_device(query_matrix, key_matrix, value_matrix, doc_ids, out_weight):
    tok_rows = query_matrix.shape[0]
    query_heads = query_matrix.shape[1] // HEAD_SIZE
    members = lax.axis_size("tp")
    core = lax.axis_index("core")
    ctx_index = lax.axis_index("z") * CORES + core
    weight_blocks = lax.all_gather(out_weight, "z", axis=0, tiled=False)
    given_pos = ctx_index * tok_rows + jnp.arange(tok_rows, dtype=jnp.int32)
    info = ctx_index.astype(jnp.int32).reshape(1)
    docs = doc_ids.reshape(-1, tok_rows)
    vmem = pl.BlockSpec(memory_space=pltpu.VMEM)
    smem = pl.BlockSpec(memory_space=pltpu.SMEM)
    small = pltpu.CompilerParams(vmem_limit_bytes=16 * 2**20)
    chips = lax.axis_size("z")
    queries, here, rest_here, first = pl.pallas_call(
        functools.partial(prepare, query_heads),
        out_shape=(
            jax.ShapeDtypeStruct((query_heads, tok_rows, HEAD_SIZE), jnp.bfloat16),
            jax.ShapeDtypeStruct((tok_rows + HEAD_SIZE - REST, HEAD_SIZE), jnp.bfloat16),
            jax.ShapeDtypeStruct((chips, REST, tok_rows), jnp.bfloat16),
            jax.ShapeDtypeStruct((8, tok_rows), jnp.int32),
        ),
        in_specs=[smem] + [vmem] * 6,
        out_specs=(vmem,) * 4,
        compiler_params=small,
        cost_estimate=pl.CostEstimate(flops=10**6, bytes_accessed=10**6, transcendentals=0),
        name="prepare",
    )(info, *rotary_tables(given_pos), query_matrix, key_matrix, value_matrix, docs)
    swap = [(i, CORES - 1 - i) for i in range(CORES)]
    most_a = lax.all_gather(here, "z", axis=0, tiled=False)
    most_b = lax.ppermute(most_a, "core", swap)
    rest_a = lax.all_to_all(rest_here, "z", split_axis=0, concat_axis=0, tiled=True)
    rest_b = lax.ppermute(rest_a, "core", swap)
    together = 1
    sets = query_heads // together
    attention = pl.pallas_call(
        functools.partial(attend, query_heads, together),
        out_shape=jax.ShapeDtypeStruct((tok_rows, query_heads * HEAD_SIZE), jnp.bfloat16),
        in_specs=[smem] + [vmem] * 6,
        out_specs=vmem,
        scratch_shapes=[
            pltpu.VMEM((sets, 1, together * tok_rows), jnp.float32),
            pltpu.VMEM((sets, 1, together * tok_rows), jnp.float32),
            pltpu.VMEM((sets, HEAD_SIZE, together * tok_rows), jnp.float32),
        ],
        cost_estimate=pl.CostEstimate(flops=2 * 10**9, bytes_accessed=3 * 10**6, transcendentals=10**6),
        compiler_params=small,
        name="attend",
    )(info, first, queries, most_a, most_b, rest_a, rest_b)
    attention_other = lax.ppermute(attention, "core", swap)
    blocks, depth, width = weight_blocks.shape
    share = blocks // members
    terms = pl.pallas_call(
        functools.partial(project, share),
        out_shape=jax.ShapeDtypeStruct((members, CORES * tok_rows, share * width), jnp.bfloat16),
        in_specs=[vmem, vmem, pl.BlockSpec(memory_space=pltpu.HBM)],
        out_specs=vmem,
        scratch_shapes=[
            pltpu.VMEM(weight_blocks.shape, jnp.bfloat16),
            pltpu.SemaphoreType.DMA((members,)),
        ],
        compiler_params=pltpu.CompilerParams(vmem_limit_bytes=59 * 2**20),
        cost_estimate=pl.CostEstimate(flops=10**9, bytes_accessed=10**7, transcendentals=0),
        name="project",
    )(attention, attention_other, weight_blocks)
    arrived = lax.all_to_all(terms, "tp", split_axis=0, concat_axis=0, tiled=True)
    half = jax.ShapeDtypeStruct((tok_rows, share * width), jnp.bfloat16)
    kept, sent = pl.pallas_call(
        total,
        out_shape=(half, half),
        in_specs=[vmem],
        out_specs=(vmem, vmem),
        compiler_params=small,
        name="total",
    )(arrived)
    given = lax.ppermute(sent, "core", swap)
    return pl.pallas_call(
        functools.partial(weave, share),
        out_shape=jax.ShapeDtypeStruct((tok_rows, share * CORES * width), jnp.bfloat16),
        in_specs=[pl.BlockSpec(memory_space=pltpu.SMEM), vmem, vmem],
        out_specs=vmem,
        compiler_params=small,
        name="weave",
    )(core.astype(jnp.int32).reshape(1), kept, given)


def solution(mesh):
    groups, ctx, tp = mesh.devices.shape
    fine = Mesh(mesh.devices.reshape(groups, ctx // CORES, CORES, tp), ("groups", "z", "core", "tp"))
    tokens = ("groups", "z", "core")
    in_specs = (P(tokens, "tp"), P(tokens, "tp"), P(tokens, "tp"), P("groups"), P("tp", ("z", "core")))
    return jax.shard_map(
        on_device, mesh=fine, in_specs=in_specs, out_specs=P(tokens, "tp"), check_vma=False
    )
```
